32 devices in a mesh: groups: 2 (over y), seq: 8 (over z, x), sub: 2 (over core).
Axes of the slice: x: 2, y: 2, z: 4, core: 2. Of those that a mesh axis runs over, the one named last changes fastest.
Arguments:
- cache_in: bfloat16 [64, 2, 36864], P('groups', None, ('sub', 'seq')), parts along dimension 0, may hold values from -6 to 6
- page_counts: int32 [16], P('groups'), parts along dimension 0, may hold values from 1 to 8, 32 in all
- tail_tokens: int32 [16], P('groups'), parts along dimension 0, may hold values from 1 to 64
- assignment: int32 [16], P('groups'), parts along dimension 0, may hold values from 0 to 7, each once
Outputs:
- cache_out: bfloat16 [128, 2, 36864], P(('groups', 'seq'), None, 'sub'), parts along dimension 0
- checksum: float32 [2, 128], P(None, ('groups', 'seq')), parts along dimension 1
The draws below stay inside these ranges and needn't reach their ends.
There are 2 independent parts, one for each index of `groups`. The reference program is written for one: setup_inputs(seed, part) draws one part's arguments, and reference() takes and returns one part's arrays. A program takes and returns all parts, laid end to end along the dimension named above; each array names one. Nothing has to cross between parts.
Inputs may be any that keep to these rules, and one draw needn't show every extreme that they name: `page_counts`: the page counts sum to 32. `assignment`: every seq index serves exactly one request.
All inputs are finite; a program needn't handle non-finite values.
Results may differ from the reference program's by a relative error of at most 0.001.
Values may be sent and summed in bfloat16 or wider, within the bound.
A program may use at most 64 MiB of HBM per device.

```python
import math
import jax
import jax.numpy as jnp
import numpy as np
from jax import lax

LATENT = 576
PAGE = 64
LAYERS = 2
MAXP = 8
REQS = 8
PAGES = 32
SLOTS = 64
ROW = 36864
N_SEQ = 8


def touch_ends(entries, rng, smallest, largest):
    spot = [jax.random.randint(jax.random.fold_in(rng, axis), (), 0, length) for axis, length in enumerate(entries.shape)]
    longest = entries.shape.index(max(entries.shape))
    beside = spot[:longest] + [(spot[longest] + 1) % entries.shape[longest]] + spot[longest + 1:]
    return entries.at[tuple(spot)].set(smallest).at[tuple(beside)].set(largest)


def steps_of(rng, dims, pieces, smallest, high):
    def one(axis_at, blocks):
        draws = jax.random.uniform(jax.random.fold_in(jax.random.fold_in(rng, 6), axis_at), (blocks,), jnp.float32, smallest / len(pieces), high / len(pieces))
        return jnp.repeat(jnp.exp(draws), dims[axis_at] // blocks).reshape((-1,) + (1,) * (len(dims) - axis_at - 1))

    level = one(*pieces[0])
    for cut in pieces[1:]:
        level = level * one(*cut)
    return level


def profile(amount, total, bound, skew):
    weights = [(1 << 20) // math.isqrt(standing ** skew) + 1 for standing in range(2, amount + 1)]
    spare, counts = total - bound - (amount - 1), [1] * (amount - 1)
    while spare > 0:
        free = [i for i in range(amount - 1) if counts[i] < bound]
        mass, budget = sum([weights[i] for i in free]), spare
        for i in free:
            extra = min(bound - counts[i], max(1, budget * weights[i] // mass), spare)
            counts[i] = counts[i] + extra
            spare = spare - extra
    return np.array([bound] + counts)


def ragged_sizes(key, amount, total, reach, slope):
    if amount == 2:
        one = jax.random.randint(key, (), max(1, total - reach), min(reach, total - 1) + 1)
        return jnp.stack([one, total - one])
    sizes = jnp.asarray(profile(amount, total, reach, slope), jnp.int32)
    pairs = (amount - 1) // 2
    giver, receiver = sizes[1:1 + 2 * pairs:2], sizes[2:2 + 2 * pairs:2]
    margin = jnp.minimum(giver - 1, reach - receiver)
    passed = jax.random.randint(jax.random.fold_in(key, 1), (pairs,), 0, 1 << 20) % (margin + 1)
    sizes = sizes.at[1:1 + 2 * pairs:2].set(giver - passed).at[2:2 + 2 * pairs:2].set(receiver + passed)
    return sizes[jax.random.permutation(jax.random.fold_in(key, 2), amount)]


def scatter_about(key, dims, deviation, most, cuts=(), kind=jnp.bfloat16):
    drawn = deviation * jax.random.normal(key, dims, jnp.float32)
    if cuts:
        drawn = drawn * steps_of(key, dims, cuts, -0.22, 0.18)
    return jnp.clip(drawn, -most, most).astype(kind)


def setup_inputs(seed: int = 0, part: int = 0) -> dict:
    arg_keys = jax.random.split(jax.random.key(seed), 5)
    own_keys = jax.random.split(jax.random.fold_in(arg_keys[4], part), 5)
    return {
        "cache_in": scatter_about(own_keys[0], (PAGES, LAYERS, ROW), 1.0, 6.0, ((2, 16),)),
        "page_counts": ragged_sizes(own_keys[1], REQS, PAGES, MAXP, 2).astype(jnp.int32),
        "tail_tokens": touch_ends(jax.random.randint(own_keys[2], (REQS,), 1, PAGE + 1), jax.random.fold_in(own_keys[2], 1), 1, PAGE).astype(jnp.int32),
        "assignment": jax.random.permutation(own_keys[3], REQS).astype(jnp.int32),
    }


def reference(cache_in, page_counts, tail_tokens, assignment):
    starts = (jnp.cumsum(page_counts) - page_counts).astype(jnp.int32)
    request_ids = jnp.arange(REQS, dtype=jnp.int32)
    owners = jnp.zeros((REQS,), jnp.int32).at[assignment].set(request_ids)
    page_ids = jnp.arange(MAXP, dtype=jnp.int32)
    token_of = jnp.arange(ROW, dtype=jnp.int32) // LATENT

    def one_device(device):
        request = owners[device]
        count = page_counts[request]
        begin = starts[request]
        tail = tail_tokens[request]
        in_use = page_ids < count
        source_rows = jnp.where(in_use, begin + page_ids, 0).astype(jnp.int32)
        filled = jnp.where(in_use, jnp.where(page_ids < count - 1, PAGE, tail), 0)
        fetched = jnp.take(cache_in, source_rows, axis=0)
        kept_mask = token_of[None, :] < filled[:, None]
        fetched = jnp.where(kept_mask[:, None, :], fetched, jnp.zeros((), cache_in.dtype))
        squares = lax.optimization_barrier(jnp.sum(jnp.square(fetched.astype(jnp.float32)), axis=2))
        return (fetched, squares)
    pages_all, squares_all = lax.map(one_device, jnp.arange(N_SEQ, dtype=jnp.int32))
    cache_out = pages_all.reshape(SLOTS, LAYERS, ROW)
    squares_all = squares_all.reshape(SLOTS, LAYERS)
    checksum = jnp.sqrt(1.0 + squares_all / ROW).T
    return (cache_out, checksum)
```

```python
import functools

import jax
import jax.numpy as jnp
from jax import lax
from jax.experimental import pallas as pl
from jax.experimental.pallas import tpu as pltpu
from jax.sharding import PartitionSpec as P

LATENT = 576
PAGE = 64
MAXP = 8
LANES = 128
ROW_CHIPS = 2
MESH = pl.DeviceIdType.MESH


def by_device(matches, values):
    return jnp.sum(jnp.where(matches, values[None, :], 0), axis=1)


def general(cache_in, page_counts, tail_tokens, assignment):
    seq_count = lax.axis_size("seq")
    own_index = lax.axis_index("seq")
    sub_index = lax.axis_index("sub")
    total_pages, layer_count, piece = cache_in.shape
    starts = jnp.cumsum(page_counts) - page_counts
    device_ids = jnp.arange(seq_count, dtype=jnp.int32)
    matches = assignment[None, :] == device_ids[:, None]
    dest_counts = by_device(matches, page_counts)
    dest_starts = by_device(matches, starts)
    dest_tails = by_device(matches, tail_tokens)
    slot_ids = jnp.arange(seq_count * MAXP, dtype=jnp.int32)
    page_rank = slot_ids % MAXP
    counts_at = jnp.repeat(dest_counts, MAXP)
    starts_at = jnp.repeat(dest_starts, MAXP)
    tails_at = jnp.repeat(dest_tails, MAXP)
    in_use = page_rank < counts_at
    source_rows = jnp.where(in_use, starts_at + page_rank, 0)
    filled = jnp.where(in_use, jnp.where(page_rank < counts_at - 1, PAGE, tails_at), 0)
    column = (sub_index * seq_count + own_index) * piece + jnp.arange(piece, dtype=jnp.int32)
    token_of = column // LATENT
    kept_mask = token_of[None, :] < filled[:, None]
    zero_value = jnp.zeros((), cache_in.dtype)
    fetched = jnp.take(cache_in, source_rows, axis=0)
    packed = jnp.where(kept_mask[:, None, :], fetched, zero_value)
    cache_out = lax.all_to_all(packed, "seq", split_axis=0, concat_axis=2, tiled=True)
    squares = jnp.sum(jnp.square(cache_out.astype(jnp.float32)), axis=2)
    squares = lax.psum(squares, "sub")
    checksum = jnp.sqrt(1.0 + squares / (PAGE * LATENT)).T
    return (cache_out, checksum)


def exchange(n, subs, counts_in, tails_in, assign_in, x_in, out, chk, send, tab, part, parts_in,
             send_sem, recv_sem, psend_sem, precv_sem, ready_sem, in_sem,
             x, counts, tails, assign):
    me = lax.axis_index("seq")
    sub = lax.axis_index("sub")
    pages, layers, piece = x.shape
    tokens = piece // LATENT
    line = n // ROW_CHIPS
    mid = line // 2
    row = ROW_CHIPS * subs
    z, col = me // ROW_CHIPS, me % ROW_CHIPS
    place_in_row = col * subs + sub
    own_id = me * subs + sub

    def device(level, spot):
        return {"seq": level * ROW_CHIPS + spot // subs, "sub": spot % subs}

    def early(level):
        return jnp.logical_and(level == mid - 1, z == mid)

    arrivals = [pltpu.make_async_copy(a, b, in_sem.at[k]) for k, (a, b) in enumerate(
        ((counts_in, counts), (tails_in, tails), (assign_in, assign), (x_in, x)))]
    for copy in arrivals:
        copy.start()
    barrier = pltpu.get_barrier_semaphore()
    for level in range(line):
        @pl.when(jnp.logical_or(level > z, early(level)))
        def _():
            for spot in range(row):
                pl.semaphore_signal(
                    barrier, inc=1, device_id=device(level, spot), device_id_type=MESH)
    for j in range(1, row):
        pl.semaphore_signal(
            barrier, inc=1, device_id=device(z, (place_in_row + j) % row), device_id_type=MESH)

    column = lax.broadcasted_iota(jnp.int32, (layers, piece), 1)
    for f in range(tokens + 1):
        tab[f] = jnp.where(column < f * LATENT, 1.0, 0.0).astype(x.dtype)

    for copy in arrivals:
        copy.wait()
    reqs = counts.shape[0]
    packed, begin = [], jnp.int32(0)
    for r in range(reqs):
        packed.append((begin * 16 + counts[r]) * 128 + tails[r])
        begin = begin + counts[r]
    base = (sub * n + me) * tokens

    for dest in range(n):
        info = jnp.int32(0)
        for r in range(reqs):
            info = info + jnp.where(assign[r] == dest, packed[r], 0)
        tail = info & 127
        count = (info >> 7) & 15
        start = info >> 11
        for k in range(MAXP):
            used = k < count
            row_at = jnp.where(used, start + k, 0)
            filled = jnp.where(used, jnp.where(k < count - 1, PAGE, tail), 0)
            keep = jnp.clip(filled - base, 0, tokens)
            send[dest, k] = x[row_at] * tab[keep]

    def columns(source):
        return out.at[:, :, pl.ds(pl.multiple_of(source * piece, LANES), piece)]

    def send_piece(level, place):
        dest = level * ROW_CHIPS + place
        pltpu.make_async_remote_copy(
            src_ref=send.at[dest],
            dst_ref=columns(me),
            send_sem=send_sem,
            recv_sem=recv_sem,
            device_id={"seq": dest},
            device_id_type=MESH).start()

    def send_part(level, spot):
        pltpu.make_async_remote_copy(
            src_ref=part.at[level * ROW_CHIPS + spot // subs],
            dst_ref=parts_in.at[own_id],
            send_sem=psend_sem,
            recv_sem=precv_sem,
            device_id=device(level, spot),
            device_id_type=MESH).start()

    pl.semaphore_wait(barrier, (z + 1) * row - 1 + jnp.where(z == mid - 1, row, 0))
    for level in range(line - 1):
        @pl.when(jnp.logical_and(level < z, jnp.logical_not(early(level))))
        def _():
            for spot in range(row):
                pl.semaphore_signal(
                    ready_sem.at[z], inc=1, device_id=device(level, spot), device_id_type=MESH)

    @pl.when(z > 0)
    def _():
        for i in range(ROW_CHIPS):
            send_piece(0, (col + i) % ROW_CHIPS)

    @pl.when(z == mid - 1)
    def _():
        send_piece(mid, col)

    lane = lax.broadcasted_iota(jnp.int32, (layers, LANES), 1)
    for dest in range(n):
        total = jnp.zeros((layers, LANES), jnp.float32)
        for k in range(MAXP):
            v = send[dest, k].astype(jnp.float32)
            s = jnp.sum(v * v, axis=1, keepdims=True)
            total = jnp.where(lane == k, s, total)
        part[dest] = total
    mine = pl.ds(pl.multiple_of(me * piece, LANES), piece)
    for k in range(MAXP):
        out[k, :, mine] = send[me, k]
    parts_in[own_id] = part[me]

    for level in range(line - 1):
        @pl.when(level < z)
        def _():
            for spot in range(row):
                send_part(level, spot)
    for j in range(1, row):
        send_part(z, (place_in_row + j) % row)

    @pl.when(z == mid - 1)
    def _():
        for spot in range(row):
            send_part(mid, spot)
        for i in range(1, ROW_CHIPS):
            send_piece(mid, (col + i) % ROW_CHIPS)

    for level in range(1, line - 1):
        @pl.when(level < z)
        def _():
            for i in range(ROW_CHIPS):
                send_piece(level, (col + i) % ROW_CHIPS)
    for i in range(1, ROW_CHIPS):
        send_piece(z, (col + i) % ROW_CHIPS)

    for level in range(1, line):
        special = jnp.logical_and(z == mid - 1, level == mid)
        @pl.when(jnp.logical_and(level > z, jnp.logical_not(special)))
        def _():
            pl.semaphore_wait(ready_sem.at[level], row)
            for spot in range(row):
                send_part(level, spot)
            for i in range(ROW_CHIPS):
                send_piece(level, (col + i) % ROW_CHIPS)

    def whole(ref, sem):
        return pltpu.make_async_copy(ref, ref, sem)

    others = n * subs - 1
    whole(parts_in.at[pl.ds(0, others)], precv_sem).wait()
    total = jnp.sum(parts_in[...], axis=0)
    chk[...] = jnp.sqrt(1.0 + total / (PAGE * LATENT))[:, :MAXP]
    whole(parts_in.at[pl.ds(0, others)], psend_sem).wait()
    whole(send.at[pl.ds(0, n - 1)], send_sem).wait()
    whole(send.at[pl.ds(0, n - 1)], recv_sem).wait()


def place(pages_in, sums_in, pages, sums, sem):
    copies = [pltpu.make_async_copy(a, b, sem.at[k]) for k, (a, b) in enumerate(
        ((pages_in, pages), (sums_in, sums)))]
    for copy in copies:
        copy.start()
    for copy in copies:
        copy.wait()


def direct(cache_in, page_counts, tail_tokens, assignment):
    n, subs = lax.axis_size("seq"), lax.axis_size("sub")
    pages, layers, piece = cache_in.shape
    vmem = pl.BlockSpec(memory_space=pltpu.VMEM)
    landed = pl.pallas_call(
        functools.partial(exchange, n, subs),
        out_shape=(pltpu.VMEM((MAXP, layers, piece * n), cache_in.dtype),
                   pltpu.VMEM((layers, MAXP), jnp.float32)),
        in_specs=[pl.BlockSpec(memory_space=pl.ANY)] * 4,
        out_specs=(vmem, vmem),
        scratch_shapes=[
            pltpu.VMEM((n, MAXP, layers, piece), cache_in.dtype),
            pltpu.VMEM((piece // LATENT + 1, layers, piece), cache_in.dtype),
            pltpu.VMEM((n, layers, LANES), jnp.float32),
            pltpu.VMEM((n * subs, layers, LANES), jnp.float32),
            pltpu.SemaphoreType.DMA,
            pltpu.SemaphoreType.DMA,
            pltpu.SemaphoreType.DMA,
            pltpu.SemaphoreType.DMA,
            pltpu.SemaphoreType.REGULAR((n // ROW_CHIPS,)),
            pltpu.SemaphoreType.DMA((4,)),
            pltpu.VMEM(cache_in.shape, cache_in.dtype),
            pltpu.SMEM(page_counts.shape, jnp.int32),
            pltpu.SMEM(page_counts.shape, jnp.int32),
            pltpu.SMEM(page_counts.shape, jnp.int32),
        ],
        compiler_params=pltpu.CompilerParams(collective_id=0, has_side_effects=True),
    )(page_counts, tail_tokens, assignment, cache_in)
    return pl.pallas_call(
        place,
        out_shape=tuple(jax.ShapeDtypeStruct(a.shape, a.dtype) for a in landed),
        in_specs=[vmem] * 2,
        out_specs=(pl.BlockSpec(memory_space=pltpu.HBM),) * 2,
        scratch_shapes=[pltpu.SemaphoreType.DMA((2,))],
    )(*(pltpu.with_memory_space_constraint(a, pltpu.VMEM) for a in landed))


def shards(cache_in, page_counts, tail_tokens, assignment):
    piece = cache_in.shape[2]
    whole_tiles = piece % LANES == 0 and piece % LATENT == 0 and lax.axis_size("seq") % ROW_CHIPS == 0
    return (direct if whole_tiles else general)(cache_in, page_counts, tail_tokens, assignment)


def solution(mesh):
    placed = (P("groups", None, ("sub", "seq")), P("groups"), P("groups"), P("groups"))
    return jax.shard_map(
        shards,
        mesh=mesh,
        in_specs=placed,
        out_specs=(P(("groups", "seq"), None, "sub"), P(None, ("groups", "seq"))),
        check_vma=False,
    )
```

```python
import functools

import jax
import jax.numpy as jnp
from jax import lax
from jax.experimental import pallas as pl
from jax.experimental.pallas import tpu as pltpu
from jax.sharding import PartitionSpec as P

LATENT = 576
PAGE = 64
MAXP = 8
LANES = 128
ROW_CHIPS = 2
NEAR_DIRECT = 8
FAR_DIRECT = 4
MESH = pl.DeviceIdType.MESH


def by_device(matches, values):
    return jnp.sum(jnp.where(matches, values[None, :], 0), axis=1)


def general(cache_in, page_counts, tail_tokens, assignment):
    seq_count = lax.axis_size("seq")
    own_index = lax.axis_index("seq")
    sub_index = lax.axis_index("sub")
    total_pages, layer_count, piece = cache_in.shape
    starts = jnp.cumsum(page_counts) - page_counts
    device_ids = jnp.arange(seq_count, dtype=jnp.int32)
    matches = assignment[None, :] == device_ids[:, None]
    dest_counts = by_device(matches, page_counts)
    dest_starts = by_device(matches, starts)
    dest_tails = by_device(matches, tail_tokens)
    slot_ids = jnp.arange(seq_count * MAXP, dtype=jnp.int32)
    page_rank = slot_ids % MAXP
    counts_at = jnp.repeat(dest_counts, MAXP)
    starts_at = jnp.repeat(dest_starts, MAXP)
    tails_at = jnp.repeat(dest_tails, MAXP)
    in_use = page_rank < counts_at
    source_rows = jnp.where(in_use, starts_at + page_rank, 0)
    filled = jnp.where(in_use, jnp.where(page_rank < counts_at - 1, PAGE, tails_at), 0)
    column = (sub_index * seq_count + own_index) * piece + jnp.arange(piece, dtype=jnp.int32)
    token_of = column // LATENT
    kept_mask = token_of[None, :] < filled[:, None]
    zero_value = jnp.zeros((), cache_in.dtype)
    fetched = jnp.take(cache_in, source_rows, axis=0)
    packed = jnp.where(kept_mask[:, None, :], fetched, zero_value)
    cache_out = lax.all_to_all(packed, "seq", split_axis=0, concat_axis=2, tiled=True)
    squares = jnp.sum(jnp.square(cache_out.astype(jnp.float32)), axis=2)
    squares = lax.psum(squares, "sub")
    checksum = jnp.sqrt(1.0 + squares / (PAGE * LATENT)).T
    return (cache_out, checksum)


def kept_direct(away):
    return FAR_DIRECT if away else NEAR_DIRECT


def most_spilled(pages, n, direct):
    half = n // 2
    room = min(pages - half, half * MAXP)
    full, rest = room // MAXP, room % MAXP
    return (MAXP - direct) * full + max(0, rest - direct)


def exchange(n, subs, counts_in, tails_in, assign_in, x_in, out, chk, send, tab, part, parts_in,
             send_sem, recv_sem, psend_sem, precv_sem, ready_sem, in_sem,
             x, counts, tails, assign, rsend_sem, spill_sem, relay, *spills):
    me = lax.axis_index("seq")
    sub = lax.axis_index("sub")
    pages, layers, piece = x.shape
    tokens = piece // LATENT
    line = n // ROW_CHIPS
    mid = line // 2
    half = mid * ROW_CHIPS
    spilled = [most_spilled(pages, n, kept_direct(away)) for away in range(mid)]
    spill, landed = spills[0], spills[1:]
    row = ROW_CHIPS * subs
    z, col = me // ROW_CHIPS, me % ROW_CHIPS
    place_in_row = col * subs + sub
    own_id = me * subs + sub
    upper = z // mid
    own_first = upper * half
    far_first = half - own_first
    relays = jnp.logical_or(z == mid - 1, z == mid)

    def device(level, spot):
        return {"seq": level * ROW_CHIPS + spot // subs, "sub": spot % subs}

    def early(level):
        return jnp.logical_and(level == mid - 1, z == mid)

    arrivals = [pltpu.make_async_copy(a, b, in_sem.at[k]) for k, (a, b) in enumerate(
        ((counts_in, counts), (tails_in, tails), (assign_in, assign), (x_in, x)))]
    for copy in arrivals:
        copy.start()
    barrier = pltpu.get_barrier_semaphore()
    for level in range(line):
        @pl.when(jnp.logical_or(level > z, early(level)))
        def _():
            for spot in range(row):
                pl.semaphore_signal(
                    barrier, inc=1, device_id=device(level, spot), device_id_type=MESH)
    for j in range(1, row):
        pl.semaphore_signal(
            barrier, inc=1, device_id=device(z, (place_in_row + j) % row), device_id_type=MESH)

    column = lax.broadcasted_iota(jnp.int32, (layers, piece), 1)
    for f in range(tokens + 1):
        tab[f] = jnp.where(column < f * LATENT, 1.0, 0.0).astype(x.dtype)
    for away in range(mid):
        landed[away][spilled[away]] = jnp.zeros((layers, piece), x.dtype)

    for copy in arrivals:
        copy.wait()
    reqs = counts.shape[0]
    packed, begin = [], jnp.int32(0)
    for r in range(reqs):
        packed.append((begin * 16 + counts[r]) * 128 + tails[r])
        begin = begin + counts[r]
    base = (sub * n + me) * tokens

    def request_of(dest):
        info = jnp.int32(0)
        for r in range(reqs):
            info = info + jnp.where(assign[r] == dest, packed[r], 0)
        return info

    for dest in range(n):
        info = request_of(dest)
        tail = info & 127
        count = (info >> 7) & 15
        start = info >> 11
        for k in range(MAXP):
            used = k < count
            row_at = jnp.where(used, start + k, 0)
            filled = jnp.where(used, jnp.where(k < count - 1, PAGE, tail), 0)
            keep = jnp.clip(filled - base, 0, tokens)
            send[dest * MAXP + k] = x[row_at] * tab[keep]

    def whole(ref, sem):
        return pltpu.make_async_copy(ref, ref, sem)

    def away_of(level):
        return level - mid if level >= mid else mid - 1 - level

    def spill_starts(first, direct):
        starts, begin = [], jnp.int32(0)
        for j in range(half):
            count = (request_of(first + j) >> 7) & 15
            starts.append((begin, count))
            begin = begin + jnp.maximum(count - direct, 0)
        return starts

    for level in range(line):
        size, direct = spilled[away_of(level)], kept_direct(away_of(level))
        if not size:
            continue

        @pl.when(z == level)
        def _():
            far = spill_starts(far_first, direct)
            for o in range(size):
                at = direct + o
                for j in range(1, half):
                    at = jnp.where(o >= far[j][0], j * MAXP + direct + o - far[j][0], at)
                spill[o] = send[far_first * MAXP + jnp.minimum(at, half * MAXP - 1)]

    def columns(source, first=0, rows=MAXP):
        return out.at[pl.ds(first, rows), :, pl.ds(pl.multiple_of(source * piece, LANES), piece)]

    def rows_to(zz, level):
        return MAXP if zz // mid == level // mid else kept_direct(away_of(zz))

    def send_piece(zz, level, turn):
        place = turn if level == 0 else (col + 1 + sub + turn) % ROW_CHIPS
        dest = level * ROW_CHIPS + place
        rows = rows_to(zz, level)
        pltpu.make_async_remote_copy(
            src_ref=send.at[pl.ds(dest * MAXP, rows)],
            dst_ref=columns(me, 0, rows),
            send_sem=send_sem,
            recv_sem=recv_sem,
            device_id={"seq": dest},
            device_id_type=MESH).start()

    def send_row(zz, level):
        for turn in range(ROW_CHIPS):
            send_piece(zz, level, turn)

    def send_spill(zz, level):
        away = away_of(zz)
        if spilled[away]:
            pltpu.make_async_remote_copy(
                src_ref=spill.at[pl.ds(0, spilled[away])],
                dst_ref=landed[away].at[pl.ds(0, spilled[away])],
                send_sem=send_sem,
                recv_sem=spill_sem.at[away],
                device_id={"seq": level * ROW_CHIPS + col},
                device_id_type=MESH).start()

    def send_part(level, spot):
        pltpu.make_async_remote_copy(
            src_ref=part.at[level * ROW_CHIPS + spot // subs],
            dst_ref=parts_in.at[own_id],
            send_sem=psend_sem,
            recv_sem=precv_sem,
            device_id=device(level, spot),
            device_id_type=MESH).start()

    def send_parts(level):
        for spot in range(row):
            send_part(level, spot)

    def sends_first(zz):
        if zz >= mid:
            send_spill(zz, mid - 1)
        if zz == mid - 1:
            send_spill(zz, mid)
        if zz >= mid:
            send_row(zz, 0)
        if zz == mid - 1:
            send_row(zz, mid)

    def sends_later(zz):
        for level in range(zz):
            send_parts(level)
        for j in range(1, row):
            send_part(zz, (place_in_row + j) % row)
        dest = zz * ROW_CHIPS + (col + 1) % ROW_CHIPS
        pltpu.make_async_remote_copy(
            src_ref=send.at[pl.ds(dest * MAXP, MAXP)],
            dst_ref=columns(me),
            send_sem=send_sem,
            recv_sem=recv_sem,
            device_id={"seq": dest},
            device_id_type=MESH).start()
        if zz == mid - 1:
            send_parts(mid)
        if 0 < zz < mid:
            send_row(zz, 0)
        first = mid if zz >= mid else 1
        for level in range(zz - 1, first - 1, -1):
            send_row(zz, level)
        if zz >= mid:
            for level in range(1, mid):
                send_row(zz, level)
        for level in range(zz + 1, line):
            if (zz, level) != (mid - 1, mid):
                pl.semaphore_wait(ready_sem.at[level], row)
                send_parts(level)
            if level < mid:
                send_piece(zz, level, 0)
            elif zz >= mid or level > mid:
                send_row(zz, level)
            elif zz != mid - 1:
                send_spill(zz, mid)
        for level in range(zz + 1, mid):
            send_piece(zz, level, 1)
        if zz < mid - 1:
            send_row(zz, mid)

    pl.semaphore_wait(barrier, (z + 1) * row - 1 + jnp.where(z == mid - 1, row, 0))
    for level in range(line - 1):
        @pl.when(jnp.logical_and(level < z, jnp.logical_not(early(level))))
        def _():
            for spot in range(row):
                pl.semaphore_signal(
                    ready_sem.at[z], inc=1, device_id=device(level, spot), device_id_type=MESH)

    for level in range(line):
        @pl.when(z == level)
        def _():
            sends_first(level)

    lane = lax.broadcasted_iota(jnp.int32, (layers, LANES), 1)
    for dest in range(n):
        total = jnp.zeros((layers, LANES), jnp.float32)
        for k in range(MAXP):
            v = send[dest * MAXP + k].astype(jnp.float32)
            s = jnp.sum(v * v, axis=1, keepdims=True)
            total = jnp.where(lane == k, s, total)
        part[dest] = total
    mine = pl.ds(pl.multiple_of(me * piece, LANES), piece)
    for k in range(MAXP):
        out[k, :, mine] = send[me * MAXP + k]
    parts_in[own_id] = part[me]

    for level in range(line):
        @pl.when(z == level)
        def _():
            sends_later(level)

    for away in range(mid - 1, -1, -1):
        size, direct = spilled[away], kept_direct(away)
        rest = MAXP - direct
        if not size:
            continue

        @pl.when(relays)
        def _():
            near = spill_starts(own_first, direct)
            level = jnp.where(upper == 1, mid - 1 - away, mid + away)
            source = level * ROW_CHIPS + col
            whole(landed[away].at[pl.ds(0, size)], spill_sem.at[away]).wait()
            for j in range(half):
                for k in range(rest):
                    at = jnp.where(k + direct < near[j][1], near[j][0] + k, size)
                    relay[away, j * rest + k] = landed[away][at]
            kept = columns(source, direct, rest)
            for j in range(half):
                @pl.when(own_first + j != me)
                def _():
                    pltpu.make_async_remote_copy(
                        src_ref=relay.at[away, pl.ds(j * rest, rest)],
                        dst_ref=kept,
                        send_sem=rsend_sem,
                        recv_sem=recv_sem,
                        device_id={"seq": own_first + j},
                        device_id_type=MESH).start()
            at_source = pl.ds(pl.multiple_of(source * piece, LANES), piece)
            for k in range(rest):
                out[direct + k, :, at_source] = relay[away, (me - own_first) * rest + k]

    others = n * subs - 1
    whole(parts_in.at[pl.ds(0, others)], precv_sem).wait()
    total = jnp.sum(parts_in[...], axis=0)
    chk[...] = jnp.sqrt(1.0 + total / (PAGE * LATENT))[:, :MAXP]
    whole(parts_in.at[pl.ds(0, others)], psend_sem).wait()
    for level in range(line):
        away = away_of(level)
        sent = (half - 1) * MAXP + half * kept_direct(away)
        got = (half - 1) * MAXP + half * MAXP
        if away == 0:
            got -= sum(MAXP - kept_direct(a) for a in range(mid))

        @pl.when(z == level)
        def _():
            whole(send.at[pl.ds(0, sent)], send_sem).wait()
            if spilled[away]:
                whole(spill.at[pl.ds(0, spilled[away])], send_sem).wait()
            if away == 0:
                for a in range(mid):
                    if spilled[a]:
                        whole(send.at[pl.ds(0, (half - 1) * (MAXP - kept_direct(a)))], rsend_sem).wait()
            whole(send.at[pl.ds(0, got)], recv_sem).wait()


def place(pages_in, sums_in, pages, sums, sem):
    copies = [pltpu.make_async_copy(a, b, sem.at[k]) for k, (a, b) in enumerate(
        ((pages_in, pages), (sums_in, sums)))]
    for copy in copies:
        copy.start()
    for copy in copies:
        copy.wait()


def direct(cache_in, page_counts, tail_tokens, assignment):
    n, subs = lax.axis_size("seq"), lax.axis_size("sub")
    pages, layers, piece = cache_in.shape
    mid = n // ROW_CHIPS // 2
    spilled = [most_spilled(pages, n, kept_direct(away)) for away in range(mid)]
    vmem = pl.BlockSpec(memory_space=pltpu.VMEM)
    landed = pl.pallas_call(
        functools.partial(exchange, n, subs),
        out_shape=(pltpu.VMEM((MAXP, layers, piece * n), cache_in.dtype),
                   pltpu.VMEM((layers, MAXP), jnp.float32)),
        in_specs=[pl.BlockSpec(memory_space=pl.ANY)] * 4,
        out_specs=(vmem, vmem),
        scratch_shapes=[
            pltpu.VMEM((n * MAXP, layers, piece), cache_in.dtype),
            pltpu.VMEM((piece // LATENT + 1, layers, piece), cache_in.dtype),
            pltpu.VMEM((n, layers, LANES), jnp.float32),
            pltpu.VMEM((n * subs, layers, LANES), jnp.float32),
            pltpu.SemaphoreType.DMA,
            pltpu.SemaphoreType.DMA,
            pltpu.SemaphoreType.DMA,
            pltpu.SemaphoreType.DMA,
            pltpu.SemaphoreType.REGULAR((n // ROW_CHIPS,)),
            pltpu.SemaphoreType.DMA((4,)),
            pltpu.VMEM(cache_in.shape, cache_in.dtype),
            pltpu.SMEM(page_counts.shape, jnp.int32),
            pltpu.SMEM(page_counts.shape, jnp.int32),
            pltpu.SMEM(page_counts.shape, jnp.int32),
            pltpu.SemaphoreType.DMA,
            pltpu.SemaphoreType.DMA((mid,)),
            pltpu.VMEM((mid, n // 2 * MAXP, layers, piece), cache_in.dtype),
            pltpu.VMEM((max(spilled) + 1, layers, piece), cache_in.dtype),
        ] + [pltpu.VMEM((size + 1, layers, piece), cache_in.dtype) for size in spilled],
        compiler_params=pltpu.CompilerParams(collective_id=0, has_side_effects=True),
    )(page_counts, tail_tokens, assignment, cache_in)
    return pl.pallas_call(
        place,
        out_shape=tuple(jax.ShapeDtypeStruct(a.shape, a.dtype) for a in landed),
        in_specs=[vmem] * 2,
        out_specs=(pl.BlockSpec(memory_space=pltpu.HBM),) * 2,
        scratch_shapes=[pltpu.SemaphoreType.DMA((2,))],
    )(*(pltpu.with_memory_space_constraint(a, pltpu.VMEM) for a in landed))


def shards(cache_in, page_counts, tail_tokens, assignment):
    piece = cache_in.shape[2]
    whole_tiles = piece % LANES == 0 and piece % LATENT == 0 and lax.axis_size("seq") % (2 * ROW_CHIPS) == 0
    return (direct if whole_tiles else general)(cache_in, page_counts, tail_tokens, assignment)


def solution(mesh):
    placed = (P("groups", None, ("sub", "seq")), P("groups"), P("groups"), P("groups"))
    return jax.shard_map(
        shards,
        mesh=mesh,
        in_specs=placed,
        out_specs=(P(("groups", "seq"), None, "sub"), P(None, ("groups", "seq"))),
        check_vma=False,
    )
```

```python
import functools

import jax
import jax.numpy as jnp
from jax import lax
from jax.experimental import pallas as pl
from jax.experimental.pallas import tpu as pltpu
from jax.sharding import PartitionSpec as P

LATENT = 576
PAGE = 64
MAXP = 8
LANES = 128
ROW_CHIPS = 2
NEAR_DIRECT = 8
FAR_DIRECT = 4
SPILL, RELAY = 8, 9
ORDER = [[[1, 3, 8, 7, 6, 2, 5, 4], [1, 2, 8, 6, 7, 3, 4, 5], [0, 2, 8, 6, 7, 3, 4, 5], [0, 3, 8, 7, 6, 2, 5, 4]], [[4, 5, 3, 0, 7, 6, 9, 1], [4, 5, 3, 0, 6, 7, 9, 1], [5, 4, 2, 0, 6, 7, 9, 1], [5, 4, 2, 0, 7, 6, 9, 1]], [[0, 1, 3, 2, 7, 6, 5, 9], [0, 1, 3, 2, 6, 7, 5, 9], [1, 0, 2, 3, 6, 7, 4, 9], [1, 0, 2, 3, 7, 6, 4, 9]], [[8, 0, 1, 7, 5, 4, 3, 2], [8, 0, 1, 7, 4, 5, 2, 3], [8, 0, 1, 6, 4, 5, 2, 3], [8, 0, 1, 6, 5, 4, 3, 2]]]
EARLY = [0, 1, 1, 3]
MESH = pl.DeviceIdType.MESH


def by_device(matches, values):
    return jnp.sum(jnp.where(matches, values[None, :], 0), axis=1)


def general(cache_in, page_counts, tail_tokens, assignment):
    seq_count = lax.axis_size("seq")
    own_index = lax.axis_index("seq")
    sub_index = lax.axis_index("sub")
    total_pages, layer_count, piece = cache_in.shape
    starts = jnp.cumsum(page_counts) - page_counts
    device_ids = jnp.arange(seq_count, dtype=jnp.int32)
    matches = assignment[None, :] == device_ids[:, None]
    dest_counts = by_device(matches, page_counts)
    dest_starts = by_device(matches, starts)
    dest_tails = by_device(matches, tail_tokens)
    slot_ids = jnp.arange(seq_count * MAXP, dtype=jnp.int32)
    page_rank = slot_ids % MAXP
    counts_at = jnp.repeat(dest_counts, MAXP)
    starts_at = jnp.repeat(dest_starts, MAXP)
    tails_at = jnp.repeat(dest_tails, MAXP)
    in_use = page_rank < counts_at
    source_rows = jnp.where(in_use, starts_at + page_rank, 0)
    filled = jnp.where(in_use, jnp.where(page_rank < counts_at - 1, PAGE, tails_at), 0)
    column = (sub_index * seq_count + own_index) * piece + jnp.arange(piece, dtype=jnp.int32)
    token_of = column // LATENT
    kept_mask = token_of[None, :] < filled[:, None]
    zero_value = jnp.zeros((), cache_in.dtype)
    fetched = jnp.take(cache_in, source_rows, axis=0)
    packed = jnp.where(kept_mask[:, None, :], fetched, zero_value)
    cache_out = lax.all_to_all(packed, "seq", split_axis=0, concat_axis=2, tiled=True)
    squares = jnp.sum(jnp.square(cache_out.astype(jnp.float32)), axis=2)
    squares = lax.psum(squares, "sub")
    checksum = jnp.sqrt(1.0 + squares / (PAGE * LATENT)).T
    return (cache_out, checksum)


def kept_direct(away):
    return FAR_DIRECT if away else NEAR_DIRECT


def most_spilled(pages, n, direct):
    half = n // 2
    room = min(pages - half, half * MAXP)
    full, rest = room // MAXP, room % MAXP
    return (MAXP - direct) * full + max(0, rest - direct)


def exchange(n, subs, counts_in, tails_in, assign_in, x_in, out, chk, send, tab, part, parts_in,
             send_sem, recv_sem, psend_sem, precv_sem, ready_sem, mate_sem, in_sem,
             x, counts, tails, assign, rsend_sem, spill_sem, relay, *spills):
    me = lax.axis_index("seq")
    sub = lax.axis_index("sub")
    pages, layers, piece = x.shape
    tokens = piece // LATENT
    line = n // ROW_CHIPS
    mid = line // 2
    half = mid * ROW_CHIPS
    spilled = [most_spilled(pages, n, kept_direct(away)) for away in range(mid)]
    spill, landed = spills[0], spills[1:]
    row = ROW_CHIPS * subs
    z, col = me // ROW_CHIPS, me % ROW_CHIPS
    place_in_row = col * subs + sub
    own_id = me * subs + sub
    upper = z // mid
    own_first = upper * half
    far_first = half - own_first
    central = jnp.logical_or(z == mid - 1, z == mid)

    def device(level, spot):
        return {"seq": level * ROW_CHIPS + spot // subs, "sub": spot % subs}

    arrivals = [pltpu.make_async_copy(a, b, in_sem.at[k]) for k, (a, b) in enumerate(
        ((counts_in, counts), (tails_in, tails), (assign_in, assign), (x_in, x)))]
    for copy in arrivals:
        copy.start()
    barrier = pltpu.get_barrier_semaphore()
    def greet(level, spot):
        pl.semaphore_signal(
            barrier, inc=1, device_id=device(level, spot), device_id_type=MESH)

    for level in range(line):
        @pl.when(z < level)
        def _():
            for spot in range(subs if level == mid else row):
                greet(level, spot + col * subs if level == mid else spot)

    @pl.when(z == mid)
    def _():
        for spot in range(subs):
            greet(mid - 1, col * subs + spot)
        for j in range(1, subs):
            greet(z, col * subs + (sub + j) % subs)

    @pl.when(z != mid)
    def _():
        for j in range(1, row):
            greet(z, (place_in_row + j) % row)

    column = lax.broadcasted_iota(jnp.int32, (layers, piece), 1)
    for f in range(tokens + 1):
        tab[f] = jnp.where(column < f * LATENT, 1.0, 0.0).astype(x.dtype)
    for away in range(mid):
        landed[away][spilled[away]] = jnp.zeros((layers, piece), x.dtype)

    for copy in arrivals:
        copy.wait()
    reqs = counts.shape[0]
    packed, begin = [], jnp.int32(0)
    for r in range(reqs):
        packed.append((begin * 16 + counts[r]) * 128 + tails[r])
        begin = begin + counts[r]
    base = (sub * n + me) * tokens

    def request_of(dest):
        info = jnp.int32(0)
        for r in range(reqs):
            info = info + jnp.where(assign[r] == dest, packed[r], 0)
        return info

    ahead = jnp.where(z == mid - 1, half, 0) + jnp.where(central, col, 0)

    def fill(turn):
        dest = (ahead + turn) % n
        info = request_of(dest)
        tail = info & 127
        count = (info >> 7) & 15
        start = info >> 11
        for k in range(MAXP):
            used = k < count
            row_at = jnp.where(used, start + k, 0)
            filled = jnp.where(used, jnp.where(k < count - 1, PAGE, tail), 0)
            keep = jnp.clip(filled - base, 0, tokens)
            send[dest * MAXP + k] = x[row_at] * tab[keep]

    def whole(ref, sem):
        return pltpu.make_async_copy(ref, ref, sem)

    def away_of(level):
        return level - mid if level >= mid else mid - 1 - level

    def spill_starts(first, direct):
        starts, begin = [], jnp.int32(0)
        for j in range(half):
            count = (request_of(first + j) >> 7) & 15
            starts.append((begin, count))
            begin = begin + jnp.maximum(count - direct, 0)
        return starts

    def columns(source, first=0, rows=MAXP):
        return out.at[pl.ds(first, rows), :, pl.ds(pl.multiple_of(source * piece, LANES), piece)]

    def rows_to(zz, level):
        return MAXP if zz // mid == level // mid else kept_direct(away_of(zz))

    def send_piece(zz, level, place):
        dest = level * ROW_CHIPS + place
        rows = rows_to(zz, level)
        pltpu.make_async_remote_copy(
            src_ref=send.at[pl.ds(dest * MAXP, rows)],
            dst_ref=columns(me, 0, rows),
            send_sem=send_sem,
            recv_sem=recv_sem,
            device_id={"seq": dest},
            device_id_type=MESH).start()

    def send_row(zz, level):
        for turn in range(ROW_CHIPS):
            send_piece(zz, level, (col + 1 + sub + turn) % ROW_CHIPS)

    def send_spill(zz, level):
        away = away_of(zz)
        if spilled[away]:
            pltpu.make_async_remote_copy(
                src_ref=spill.at[pl.ds(0, spilled[away])],
                dst_ref=landed[away].at[pl.ds(0, spilled[away])],
                send_sem=send_sem,
                recv_sem=spill_sem.at[away],
                device_id={"seq": level * ROW_CHIPS + col},
                device_id_type=MESH).start()

    def send_part(level, spot):
        pltpu.make_async_remote_copy(
            src_ref=part.at[level * ROW_CHIPS + spot // subs],
            dst_ref=parts_in.at[own_id],
            send_sem=psend_sem,
            recv_sem=precv_sem,
            device_id=device(level, spot),
            device_id_type=MESH).start()

    def send_parts(level):
        for spot in range(row):
            send_part(level, spot)

    def tell_lower():
        for level in range(line - 1):
            @pl.when(jnp.logical_and(level < z, jnp.logical_not(jnp.logical_and(level == mid - 1, z == mid))))
            def _():
                for spot in range(row):
                    pl.semaphore_signal(
                        ready_sem.at[z], inc=1, device_id=device(level, spot), device_id_type=MESH)

    def send_mate(zz):
        dest = zz * ROW_CHIPS + (col + 1) % ROW_CHIPS
        pltpu.make_async_remote_copy(
            src_ref=send.at[pl.ds(dest * MAXP, MAXP)],
            dst_ref=columns(me),
            send_sem=send_sem,
            recv_sem=recv_sem,
            device_id={"seq": dest},
            device_id_type=MESH).start()

    def forward(away):
        size, direct = spilled[away], kept_direct(away)
        rest = MAXP - direct
        if not size:
            return

        near = spill_starts(own_first, direct)
        level = jnp.where(upper == 1, mid - 1 - away, mid + away)
        source = level * ROW_CHIPS + col
        whole(landed[away].at[pl.ds(0, size)], spill_sem.at[away]).wait()
        for j in range(half):
            for k in range(rest):
                at = jnp.where(k + direct < near[j][1], near[j][0] + k, size)
                relay[away, j * rest + k] = landed[away][at]
        kept = columns(source, direct, rest)
        for j in range(half):
            @pl.when(own_first + j != me)
            def _():
                pltpu.make_async_remote_copy(
                    src_ref=relay.at[away, pl.ds(j * rest, rest)],
                    dst_ref=kept,
                    send_sem=rsend_sem,
                    recv_sem=recv_sem,
                    device_id={"seq": own_first + j},
                    device_id_type=MESH).start()
        at_source = pl.ds(pl.multiple_of(source * piece, LANES), piece)
        for k in range(rest):
            out[direct + k, :, at_source] = relay[away, (me - own_first) * rest + k]

    def issue(zz, item):
        if item == SPILL:
            send_spill(zz, mid - 1 if zz >= mid else mid)
        elif item == RELAY:
            for away in range(mid - 1, -1, -1):
                forward(away)
        elif item // ROW_CHIPS == zz:
            send_mate(zz)
        else:
            send_piece(zz, item // ROW_CHIPS, item % ROW_CHIPS)

    def issue_early(zz):
        for s in range(row):
            @pl.when(jnp.logical_and(z == zz, place_in_row == s))
            def _():
                for item in ORDER[zz][s][:EARLY[zz]]:
                    issue(zz, item)

    def sends_later(zz):
        for level in range(zz):
            send_parts(level)
        if zz == mid:
            for j in range(1, subs):
                send_part(zz, col * subs + (sub + j) % subs)
        else:
            for j in range(1, row):
                send_part(zz, (place_in_row + j) % row)
        if zz == mid - 1:
            send_parts(mid)
        for s in range(row):
            @pl.when(place_in_row == s)
            def _():
                known = zz + 1 if zz == mid - 1 else zz
                for item in ORDER[zz][s][EARLY[zz]:]:
                    target = zz if item == RELAY else mid if item == SPILL and zz < mid else 0 if item == SPILL else item // ROW_CHIPS
                    if (zz, target) == (mid, mid) and item != RELAY:
                        target = mid + 1
                    while known < target:
                        known += 1
                        if (zz, known) != (mid - 1, mid):
                            pl.semaphore_wait(ready_sem.at[known], row)
                            send_parts(known)
                            if (zz, known) == (mid, mid + 1):
                                for spot in range(subs):
                                    send_part(zz, (1 - col) * subs + spot)
                    issue(zz, item)

    for turn in range(2):
        fill(turn)
    greeted = z * row + row - 1 + jnp.where(z == mid - 1, subs, 0)
    pl.semaphore_wait(barrier, jnp.where(z == mid, z * subs + subs - 1, greeted))

    for level in (mid - 1, mid):
        issue_early(level)

    @pl.when(z == mid - 1)
    def _():
        for spot in range(subs):
            for level, place in ((mid, col), (mid - 1, 1 - col)):
                pl.semaphore_signal(
                    mate_sem, inc=1, device_id=device(level, place * subs + spot),
                    device_id_type=MESH)

    @pl.when(z != mid)
    def _():
        tell_lower()

    for turn in range(2, n):
        fill(turn)

    for level in range(line):
        size, direct = spilled[away_of(level)], kept_direct(away_of(level))
        if not size:
            continue

        @pl.when(z == level)
        def _():
            far = spill_starts(far_first, direct)
            for o in range(size):
                at = direct + o
                for j in range(1, half):
                    at = jnp.where(o >= far[j][0], j * MAXP + direct + o - far[j][0], at)
                spill[o] = send[far_first * MAXP + jnp.minimum(at, half * MAXP - 1)]

    for level in range(line):
        if level not in (mid - 1, mid):
            issue_early(level)

    lane = lax.broadcasted_iota(jnp.int32, (layers, LANES), 1)
    for dest in range(n):
        total = jnp.zeros((layers, LANES), jnp.float32)
        for k in range(MAXP):
            v = send[dest * MAXP + k].astype(jnp.float32)
            s = jnp.sum(v * v, axis=1, keepdims=True)
            total = jnp.where(lane == k, s, total)
        part[dest] = total
    mine = pl.ds(pl.multiple_of(me * piece, LANES), piece)
    for k in range(MAXP):
        out[k, :, mine] = send[me * MAXP + k]
    parts_in[own_id] = part[me]

    @pl.when(central)
    def _():
        pl.semaphore_wait(mate_sem, subs)

    @pl.when(z == mid)
    def _():
        tell_lower()

    for level in range(line):
        @pl.when(z == level)
        def _():
            sends_later(level)

    others = n * subs - 1
    whole(parts_in.at[pl.ds(0, others)], precv_sem).wait()
    total = jnp.sum(parts_in[...], axis=0)
    chk[...] = jnp.sqrt(1.0 + total / (PAGE * LATENT))[:, :MAXP]
    whole(parts_in.at[pl.ds(0, others)], psend_sem).wait()
    for level in range(line):
        away = away_of(level)
        sent = (half - 1) * MAXP + half * kept_direct(away)
        got = (half - 1) * MAXP + half * MAXP
        if away == 0:
            got -= sum(MAXP - kept_direct(a) for a in range(mid))

        @pl.when(z == level)
        def _():
            whole(send.at[pl.ds(0, sent)], send_sem).wait()
            if spilled[away]:
                whole(spill.at[pl.ds(0, spilled[away])], send_sem).wait()
            if away == 0:
                for a in range(mid):
                    if spilled[a]:
                        whole(send.at[pl.ds(0, (half - 1) * (MAXP - kept_direct(a)))], rsend_sem).wait()
            whole(send.at[pl.ds(0, got)], recv_sem).wait()


def place(pages_in, sums_in, pages, sums, sem):
    copies = [pltpu.make_async_copy(a, b, sem.at[k]) for k, (a, b) in enumerate(
        ((pages_in, pages), (sums_in, sums)))]
    for copy in copies:
        copy.start()
    for copy in copies:
        copy.wait()


def direct(cache_in, page_counts, tail_tokens, assignment):
    n, subs = lax.axis_size("seq"), lax.axis_size("sub")
    pages, layers, piece = cache_in.shape
    mid = n // ROW_CHIPS // 2
    spilled = [most_spilled(pages, n, kept_direct(away)) for away in range(mid)]
    vmem = pl.BlockSpec(memory_space=pltpu.VMEM)
    landed = pl.pallas_call(
        functools.partial(exchange, n, subs),
        out_shape=(pltpu.VMEM((MAXP, layers, piece * n), cache_in.dtype),
                   pltpu.VMEM((layers, MAXP), jnp.float32)),
        in_specs=[pl.BlockSpec(memory_space=pl.ANY)] * 4,
        out_specs=(vmem, vmem),
        scratch_shapes=[
            pltpu.VMEM((n * MAXP, layers, piece), cache_in.dtype),
            pltpu.VMEM((piece // LATENT + 1, layers, piece), cache_in.dtype),
            pltpu.VMEM((n, layers, LANES), jnp.float32),
            pltpu.VMEM((n * subs, layers, LANES), jnp.float32),
            pltpu.SemaphoreType.DMA,
            pltpu.SemaphoreType.DMA,
            pltpu.SemaphoreType.DMA,
            pltpu.SemaphoreType.DMA,
            pltpu.SemaphoreType.REGULAR((n // ROW_CHIPS,)),
            pltpu.SemaphoreType.REGULAR,
            pltpu.SemaphoreType.DMA((4,)),
            pltpu.VMEM(cache_in.shape, cache_in.dtype),
            pltpu.SMEM(page_counts.shape, jnp.int32),
            pltpu.SMEM(page_counts.shape, jnp.int32),
            pltpu.SMEM(page_counts.shape, jnp.int32),
            pltpu.SemaphoreType.DMA,
            pltpu.SemaphoreType.DMA((mid,)),
            pltpu.VMEM((mid, n // 2 * MAXP, layers, piece), cache_in.dtype),
            pltpu.VMEM((max(spilled) + 1, layers, piece), cache_in.dtype),
        ] + [pltpu.VMEM((size + 1, layers, piece), cache_in.dtype) for size in spilled],
        compiler_params=pltpu.CompilerParams(collective_id=0, has_side_effects=True),
    )(page_counts, tail_tokens, assignment, cache_in)
    return pl.pallas_call(
        place,
        out_shape=tuple(jax.ShapeDtypeStruct(a.shape, a.dtype) for a in landed),
        in_specs=[vmem] * 2,
        out_specs=(pl.BlockSpec(memory_space=pltpu.HBM),) * 2,
        scratch_shapes=[pltpu.SemaphoreType.DMA((2,))],
    )(*(pltpu.with_memory_space_constraint(a, pltpu.VMEM) for a in landed))


def shards(cache_in, page_counts, tail_tokens, assignment):
    piece = cache_in.shape[2]
    whole_tiles = piece % LANES == 0 and piece % LATENT == 0 and lax.axis_size("seq") == len(ORDER) * ROW_CHIPS
    return (direct if whole_tiles else general)(cache_in, page_counts, tail_tokens, assignment)


def solution(mesh):
    placed = (P("groups", None, ("sub", "seq")), P("groups"), P("groups"), P("groups"))
    return jax.shard_map(
        shards,
        mesh=mesh,
        in_specs=placed,
        out_specs=(P(("groups", "seq"), None, "sub"), P(None, ("groups", "seq"))),
        check_vma=False,
    )
```

```python
import functools
import math

import jax
import jax.numpy as jnp
from jax import lax
from jax.experimental import pallas as pl
from jax.experimental.pallas import tpu as pltpu
from jax.sharding import PartitionSpec as P

LATENT = 576
PAGE = 64
MAXP = 8
LANES = 128
ROW_CHIPS = 2
DIRECT = 4
SPILL, RELAY = 8, 9
ORDER = [
    [[1, 3, 8, 7, 6, 2, 5, 4], [1, 2, 8, 6, 7, 3, 4, 5], [0, 2, 8, 6, 7, 3, 4, 5], [0, 3, 8, 7, 6, 2, 5, 4]],
    [[4, 5, 3, 0, 7, 6, 9, 1], [4, 5, 3, 0, 6, 7, 9, 1], [5, 4, 2, 0, 6, 7, 9, 1], [5, 4, 2, 0, 7, 6, 9, 1]],
    [[0, 1, 3, 2, 7, 6, 5, 9], [0, 1, 3, 2, 6, 7, 5, 9], [1, 0, 2, 3, 6, 7, 4, 9], [1, 0, 2, 3, 7, 6, 4, 9]],
    [[8, 0, 1, 7, 5, 4, 3, 2], [8, 0, 1, 7, 4, 5, 2, 3], [8, 0, 1, 6, 4, 5, 2, 3], [8, 0, 1, 6, 5, 4, 3, 2]],
]
EARLY = [0, 1, 1, 3]
MESH = pl.DeviceIdType.MESH


def by_device(matches, values):
    return jnp.sum(jnp.where(matches, values[None, :], 0), axis=1)


def general(cache_in, page_counts, tail_tokens, assignment):
    seq_count = lax.axis_size("seq")
    own_index = lax.axis_index("seq")
    sub_index = lax.axis_index("sub")
    total_pages, layer_count, piece = cache_in.shape
    starts = jnp.cumsum(page_counts) - page_counts
    device_ids = jnp.arange(seq_count, dtype=jnp.int32)
    matches = assignment[None, :] == device_ids[:, None]
    dest_counts = by_device(matches, page_counts)
    dest_starts = by_device(matches, starts)
    dest_tails = by_device(matches, tail_tokens)
    slot_ids = jnp.arange(seq_count * MAXP, dtype=jnp.int32)
    page_rank = slot_ids % MAXP
    counts_at = jnp.repeat(dest_counts, MAXP)
    starts_at = jnp.repeat(dest_starts, MAXP)
    tails_at = jnp.repeat(dest_tails, MAXP)
    in_use = page_rank < counts_at
    source_rows = jnp.where(in_use, starts_at + page_rank, 0)
    filled = jnp.where(in_use, jnp.where(page_rank < counts_at - 1, PAGE, tails_at), 0)
    column = (sub_index * seq_count + own_index) * piece + jnp.arange(piece, dtype=jnp.int32)
    token_of = column // LATENT
    kept_mask = token_of[None, :] < filled[:, None]
    zero_value = jnp.zeros((), cache_in.dtype)
    fetched = jnp.take(cache_in, source_rows, axis=0)
    packed = jnp.where(kept_mask[:, None, :], fetched, zero_value)
    cache_out = lax.all_to_all(packed, "seq", split_axis=0, concat_axis=2, tiled=True)
    squares = jnp.sum(jnp.square(cache_out.astype(jnp.float32)), axis=2)
    squares = lax.psum(squares, "sub")
    checksum = jnp.sqrt(1.0 + squares / (PAGE * LATENT)).T
    return (cache_out, checksum)


def kept_direct(away):
    return DIRECT if away else MAXP


def most_spilled(pages, n):
    half = n // 2
    full, rest = divmod(min(pages - half, half * MAXP), MAXP)
    return (MAXP - DIRECT) * full + max(0, rest - DIRECT)


def exchange(n, subs, counts_in, tails_in, assign_in, x_in, out, chk, send, tab, part, parts_in,
             send_sem, recv_sem, precv_sem, ready_sem, mate_sem,
             x, counts, tails, assign, spill_sem, relay, spill, *landed):
    me = lax.axis_index("seq")
    sub = lax.axis_index("sub")
    pages, layers, piece = x.shape
    tokens = piece // LATENT
    line = n // ROW_CHIPS
    mid = line // 2
    half = mid * ROW_CHIPS
    spilled = spill.shape[0]
    rest = MAXP - DIRECT
    row = ROW_CHIPS * subs
    z, col = me // ROW_CHIPS, me % ROW_CHIPS
    place_in_row = col * subs + sub
    own_id = me * subs + sub
    upper = z // mid
    own_first = upper * half
    far_first = half - own_first
    central = jnp.logical_or(z == mid - 1, z == mid)

    def device(level, spot):
        return {"seq": level * ROW_CHIPS + spot // subs, "sub": spot % subs}

    barrier = pltpu.get_barrier_semaphore()

    def greet(level, spot):
        pl.semaphore_signal(
            barrier, inc=1, device_id=device(level, spot), device_id_type=MESH)

    @pl.when(z == mid)
    def _():
        for spot in range(subs):
            greet(mid - 1, col * subs + spot)

    arrivals = [pltpu.make_async_copy(a, b, send_sem) for a, b in (
        (counts_in, counts), (tails_in, tails), (assign_in, assign), (x_in, x))]
    cuts = math.gcd(pages, 8)
    cut = pages // cuts
    for i in range(cuts):
        part_of = pl.ds(i * cut, cut)
        pltpu.make_async_copy(x_in.at[part_of], x.at[part_of], send_sem).start()
    for copy in arrivals[:3]:
        copy.start()
    for level in range(line):
        @pl.when(z < level)
        def _():
            for spot in range(subs if level == mid else row):
                greet(level, spot + col * subs if level == mid else spot)

    @pl.when(z == mid)
    def _():
        for j in range(1, subs):
            greet(z, col * subs + (sub + j) % subs)

    @pl.when(z != mid)
    def _():
        for j in range(1, row):
            greet(z, (place_in_row + j) % row)

    column = lax.broadcasted_iota(jnp.int32, (layers, piece), 1)
    for f in range(tokens + 1):
        tab[f] = jnp.where(column < f * LATENT, 1.0, 0.0).astype(x.dtype)
    for buffer in landed:
        buffer[spilled] = jnp.zeros((layers, piece), x.dtype)

    for copy in arrivals:
        copy.wait()
    reqs = counts.shape[0]
    packed, begin = [], jnp.int32(0)
    for r in range(reqs):
        packed.append((begin * 16 + counts[r]) * 128 + tails[r])
        begin = begin + counts[r]
    base = (sub * n + me) * tokens

    def request_of(dest):
        info = jnp.int32(0)
        for r in range(reqs):
            info = info + jnp.where(assign[r] == dest, packed[r], 0)
        return info

    ahead = jnp.where(z == mid - 1, half, 0) + jnp.where(central, col, 0)

    def fill(turn):
        dest = (ahead + turn) % n
        info = request_of(dest)
        tail = info & 127
        count = (info >> 7) & 15
        start = info >> 11
        for k in range(MAXP):
            used = k < count
            row_at = jnp.where(used, start + k, 0)
            filled = jnp.where(used, jnp.where(k < count - 1, PAGE, tail), 0)
            keep = jnp.clip(filled - base, 0, tokens)
            send[dest * MAXP + k] = x[row_at] * tab[keep]

    def whole(ref, sem):
        return pltpu.make_async_copy(ref, ref, sem)

    def away_of(level):
        return level - mid if level >= mid else mid - 1 - level

    def spill_starts(first):
        starts, begin = [], jnp.int32(0)
        for j in range(half):
            count = (request_of(first + j) >> 7) & 15
            starts.append((begin, count))
            begin = begin + jnp.maximum(count - DIRECT, 0)
        return starts

    def columns(source, first=0, rows=MAXP):
        return out.at[pl.ds(first, rows), :, pl.ds(pl.multiple_of(source * piece, LANES), piece)]

    def rows_to(zz, level):
        return MAXP if zz // mid == level // mid else kept_direct(away_of(zz))

    def send_piece(zz, level, place):
        dest = level * ROW_CHIPS + place
        rows = rows_to(zz, level)
        pltpu.make_async_remote_copy(
            src_ref=send.at[pl.ds(dest * MAXP, rows)],
            dst_ref=columns(me, 0, rows),
            send_sem=send_sem,
            recv_sem=recv_sem,
            device_id={"seq": dest},
            device_id_type=MESH).start()

    def send_spill(zz):
        away = away_of(zz)
        pltpu.make_async_remote_copy(
            src_ref=spill,
            dst_ref=landed[away - 1].at[pl.ds(0, spilled)],
            send_sem=send_sem,
            recv_sem=spill_sem.at[away - 1],
            device_id={"seq": (mid - 1 if zz >= mid else mid) * ROW_CHIPS + col},
            device_id_type=MESH).start()

    def send_part(level, spot):
        pltpu.make_async_remote_copy(
            src_ref=part.at[level * ROW_CHIPS + spot // subs],
            dst_ref=parts_in.at[own_id],
            send_sem=send_sem,
            recv_sem=precv_sem,
            device_id=device(level, spot),
            device_id_type=MESH).start()

    def send_parts(level):
        for spot in range(row):
            send_part(level, spot)

    def tell_lower():
        for level in range(line - 1):
            by_entry = jnp.logical_and(level == mid - 1, z == mid)

            @pl.when(jnp.logical_and(level < z, jnp.logical_not(by_entry)))
            def _():
                for spot in range(row):
                    pl.semaphore_signal(
                        ready_sem.at[z - 1], inc=1, device_id=device(level, spot), device_id_type=MESH)

    def send_mate(zz):
        dest = zz * ROW_CHIPS + (col + 1) % ROW_CHIPS
        pltpu.make_async_remote_copy(
            src_ref=send.at[pl.ds(dest * MAXP, MAXP)],
            dst_ref=columns(me),
            send_sem=send_sem,
            recv_sem=recv_sem,
            device_id={"seq": dest},
            device_id_type=MESH).start()

    def forward(away):
        near = spill_starts(own_first)
        level = jnp.where(upper == 1, mid - 1 - away, mid + away)
        source = level * ROW_CHIPS + col
        whole(landed[away - 1].at[pl.ds(0, spilled)], spill_sem.at[away - 1]).wait()
        for j in range(half):
            for k in range(rest):
                at = jnp.where(k + DIRECT < near[j][1], near[j][0] + k, spilled)
                relay[away - 1, j * rest + k] = landed[away - 1][at]
        kept = columns(source, DIRECT, rest)
        for j in range(half):
            @pl.when(own_first + j != me)
            def _():
                pltpu.make_async_remote_copy(
                    src_ref=relay.at[away - 1, pl.ds(j * rest, rest)],
                    dst_ref=kept,
                    send_sem=send_sem,
                    recv_sem=recv_sem,
                    device_id={"seq": own_first + j},
                    device_id_type=MESH).start()
        at_source = pl.ds(pl.multiple_of(source * piece, LANES), piece)
        for k in range(rest):
            out[DIRECT + k, :, at_source] = relay[away - 1, (me - own_first) * rest + k]

    def issue(zz, item):
        if item == SPILL:
            send_spill(zz)
        elif item == RELAY:
            for away in range(mid - 1, 0, -1):
                forward(away)
        elif item // ROW_CHIPS == zz:
            send_mate(zz)
        else:
            send_piece(zz, item // ROW_CHIPS, item % ROW_CHIPS)

    def issue_early(zz):
        for s in range(row):
            @pl.when(jnp.logical_and(z == zz, place_in_row == s))
            def _():
                for item in ORDER[zz][s][:EARLY[zz]]:
                    issue(zz, item)

    def sends_later(zz):
        for level in range(zz):
            send_parts(level)
        if zz == mid:
            for j in range(1, subs):
                send_part(zz, col * subs + (sub + j) % subs)
        else:
            for j in range(1, row):
                send_part(zz, (place_in_row + j) % row)
        if zz == mid - 1:
            send_parts(mid)
        for s in range(row):
            @pl.when(place_in_row == s)
            def _():
                known = zz + 1 if zz == mid - 1 else zz
                for item in ORDER[zz][s][EARLY[zz]:]:
                    target = item // ROW_CHIPS
                    if item == RELAY:
                        target = zz
                    elif item == SPILL:
                        target = mid if zz < mid else 0
                    elif zz == target == mid:
                        target = mid + 1
                    while known < target:
                        known += 1
                        if (zz, known) != (mid - 1, mid):
                            pl.semaphore_wait(ready_sem.at[known - 1], row)
                            send_parts(known)
                            if (zz, known) == (mid, mid + 1):
                                for spot in range(subs):
                                    send_part(zz, (1 - col) * subs + spot)
                    issue(zz, item)

    def pack_rest():
        for turn in range(2, n):
            fill(turn)

        @pl.when(jnp.logical_not(central))
        def _():
            far = spill_starts(far_first)
            for o in range(spilled):
                at = DIRECT + o
                for j in range(1, half):
                    at = jnp.where(o >= far[j][0], j * MAXP + DIRECT + o - far[j][0], at)
                spill[o] = send[far_first * MAXP + jnp.minimum(at, half * MAXP - 1)]

    for turn in range(2):
        fill(turn)

    @pl.when(jnp.logical_not(central))
    def _():
        pack_rest()

    greeted = z * row + row - 1 + jnp.where(z == mid - 1, subs, 0)
    pl.semaphore_wait(barrier, jnp.where(z == mid, z * subs + subs - 1, greeted))

    for level in (mid - 1, mid):
        issue_early(level)

    @pl.when(z == mid - 1)
    def _():
        for spot in range(subs):
            for level, place in ((mid, col), (mid - 1, 1 - col)):
                pl.semaphore_signal(
                    mate_sem, inc=1, device_id=device(level, place * subs + spot),
                    device_id_type=MESH)

    @pl.when(z != mid)
    def _():
        tell_lower()

    @pl.when(central)
    def _():
        pack_rest()
    for level in range(line):
        if level not in (mid - 1, mid):
            issue_early(level)

    lane = lax.broadcasted_iota(jnp.int32, (layers, LANES), 1)
    for dest in range(n):
        total = jnp.zeros((layers, LANES), jnp.float32)
        for k in range(MAXP):
            v = send[dest * MAXP + k].astype(jnp.float32)
            s = jnp.sum(v * v, axis=1, keepdims=True)
            total = jnp.where(lane == k, s, total)
        part[dest] = total
    mine = pl.ds(pl.multiple_of(me * piece, LANES), piece)
    for k in range(MAXP):
        out[k, :, mine] = send[me * MAXP + k]
    parts_in[own_id] = part[me]

    @pl.when(central)
    def _():
        pl.semaphore_wait(mate_sem, subs)

    @pl.when(z == mid)
    def _():
        tell_lower()

    for level in range(line):
        @pl.when(z == level)
        def _():
            sends_later(level)

    others = n * subs - 1
    whole(parts_in.at[pl.ds(0, others)], precv_sem).wait()
    total = jnp.sum(parts_in[...], axis=0)
    chk[...] = jnp.sqrt(1.0 + total / (PAGE * LATENT))[:, :MAXP]
    whole(parts_in.at[pl.ds(0, others)], send_sem).wait()
    for level in range(line):
        away = away_of(level)
        forwards = 0 if away else mid - 1
        sent = (half - 1) * MAXP + half * kept_direct(away)
        got = (n - 1) * MAXP - forwards * rest

        @pl.when(z == level)
        def _():
            whole(send.at[pl.ds(0, sent)], send_sem).wait()
            if away:
                whole(spill, send_sem).wait()
            else:
                whole(send.at[pl.ds(0, forwards * (half - 1) * rest)], send_sem).wait()
            whole(send.at[pl.ds(0, got)], recv_sem).wait()


def place(pages_in, sums_in, pages, sums, sem):
    copies = [pltpu.make_async_copy(a, b, sem.at[k]) for k, (a, b) in enumerate(
        ((pages_in, pages), (sums_in, sums)))]
    for copy in copies:
        copy.start()
    for copy in copies:
        copy.wait()


def direct(cache_in, page_counts, tail_tokens, assignment):
    n, subs = lax.axis_size("seq"), lax.axis_size("sub")
    pages, layers, piece = cache_in.shape
    mid = n // ROW_CHIPS // 2
    spilled = most_spilled(pages, n)
    vmem = pl.BlockSpec(memory_space=pltpu.VMEM)
    landed = pl.pallas_call(
        functools.partial(exchange, n, subs),
        out_shape=(pltpu.VMEM((MAXP, layers, piece * n), cache_in.dtype),
                   pltpu.VMEM((layers, MAXP), jnp.float32)),
        in_specs=[pl.BlockSpec(memory_space=pl.ANY)] * 4,
        out_specs=(vmem, vmem),
        scratch_shapes=[
            pltpu.VMEM((n * MAXP, layers, piece), cache_in.dtype),
            pltpu.VMEM((piece // LATENT + 1, layers, piece), cache_in.dtype),
            pltpu.VMEM((n, layers, LANES), jnp.float32),
            pltpu.VMEM((n * subs, layers, LANES), jnp.float32),
            pltpu.SemaphoreType.DMA,
            pltpu.SemaphoreType.DMA,
            pltpu.SemaphoreType.DMA,
            pltpu.SemaphoreType.REGULAR((n // ROW_CHIPS - 1,)),
            pltpu.SemaphoreType.REGULAR,
            pltpu.VMEM(cache_in.shape, cache_in.dtype),
            pltpu.SMEM(page_counts.shape, jnp.int32),
            pltpu.SMEM(page_counts.shape, jnp.int32),
            pltpu.SMEM(page_counts.shape, jnp.int32),
            pltpu.SemaphoreType.DMA((mid - 1,)),
            pltpu.VMEM((mid - 1, n // 2 * (MAXP - DIRECT), layers, piece), cache_in.dtype),
            pltpu.VMEM((spilled, layers, piece), cache_in.dtype),
        ] + [pltpu.VMEM((spilled + 1, layers, piece), cache_in.dtype)] * (mid - 1),
        compiler_params=pltpu.CompilerParams(collective_id=0, has_side_effects=True),
    )(page_counts, tail_tokens, assignment, cache_in)
    return pl.pallas_call(
        place,
        out_shape=tuple(jax.ShapeDtypeStruct(a.shape, a.dtype) for a in landed),
        in_specs=[vmem] * 2,
        out_specs=(pl.BlockSpec(memory_space=pltpu.HBM),) * 2,
        scratch_shapes=[pltpu.SemaphoreType.DMA((2,))],
    )(*(pltpu.with_memory_space_constraint(a, pltpu.VMEM) for a in landed))


def shards(cache_in, page_counts, tail_tokens, assignment):
    pages, _, piece = cache_in.shape
    n, subs = lax.axis_size("seq"), lax.axis_size("sub")
    whole_tiles = piece % LANES == 0 and piece % LATENT == 0
    in_order = n == len(ORDER) * ROW_CHIPS and subs * ROW_CHIPS == len(ORDER[0])
    fits = in_order and page_counts.shape[0] == n
    return (direct if whole_tiles and fits else general)(cache_in, page_counts, tail_tokens, assignment)


def solution(mesh):
    placed = (P("groups", None, ("sub", "seq")), P("groups"), P("groups"), P("groups"))
    return jax.shard_map(
        shards,
        mesh=mesh,
        in_specs=placed,
        out_specs=(P(("groups", "seq"), None, "sub"), P(None, ("groups", "seq"))),
        check_vma=False,
    )
```

```python
import functools
import math

import jax
import jax.numpy as jnp
from jax import lax
from jax.experimental import pallas as pl
from jax.experimental.pallas import tpu as pltpu
from jax.sharding import PartitionSpec as P

LATENT = 576
PAGE = 64
MAXP = 8
LANES = 128
ROW_CHIPS = 2
DIRECT = 4
SPILL, RELAY = 8, 9
ORDER = [
    [[1, 3, 8, 7, 6, 2, 5, 4], [1, 2, 8, 7, 6, 3, 5, 4], [0, 2, 8, 6, 7, 3, 4, 5], [0, 3, 8, 6, 7, 2, 4, 5]],
    [[4, 5, 3, 0, 7, 6, 9, 1], [4, 5, 3, 0, 7, 6, 9, 1], [5, 4, 2, 0, 6, 7, 9, 1], [5, 4, 2, 0, 6, 7, 9, 1]],
    [[0, 1, 3, 2, 7, 6, 5, 9], [0, 1, 3, 2, 6, 7, 5, 9], [1, 0, 2, 3, 6, 7, 4, 9], [1, 0, 2, 3, 7, 6, 4, 9]],
    [[8, 0, 1, 7, 5, 4, 3, 2], [8, 0, 1, 7, 4, 5, 2, 3], [8, 0, 1, 6, 4, 5, 2, 3], [8, 0, 1, 6, 5, 4, 3, 2]],
]
EARLY = [0, 1, 1, 3]
MESH = pl.DeviceIdType.MESH


def by_device(matches, values):
    return jnp.sum(jnp.where(matches, values[None, :], 0), axis=1)


def general(cache_in, page_counts, tail_tokens, assignment):
    seq_count = lax.axis_size("seq")
    own_index = lax.axis_index("seq")
    sub_index = lax.axis_index("sub")
    total_pages, layer_count, piece = cache_in.shape
    starts = jnp.cumsum(page_counts) - page_counts
    device_ids = jnp.arange(seq_count, dtype=jnp.int32)
    matches = assignment[None, :] == device_ids[:, None]
    dest_counts = by_device(matches, page_counts)
    dest_starts = by_device(matches, starts)
    dest_tails = by_device(matches, tail_tokens)
    slot_ids = jnp.arange(seq_count * MAXP, dtype=jnp.int32)
    page_rank = slot_ids % MAXP
    counts_at = jnp.repeat(dest_counts, MAXP)
    starts_at = jnp.repeat(dest_starts, MAXP)
    tails_at = jnp.repeat(dest_tails, MAXP)
    in_use = page_rank < counts_at
    source_rows = jnp.where(in_use, starts_at + page_rank, 0)
    filled = jnp.where(in_use, jnp.where(page_rank < counts_at - 1, PAGE, tails_at), 0)
    column = (sub_index * seq_count + own_index) * piece + jnp.arange(piece, dtype=jnp.int32)
    token_of = column // LATENT
    kept_mask = token_of[None, :] < filled[:, None]
    zero_value = jnp.zeros((), cache_in.dtype)
    fetched = jnp.take(cache_in, source_rows, axis=0)
    packed = jnp.where(kept_mask[:, None, :], fetched, zero_value)
    cache_out = lax.all_to_all(packed, "seq", split_axis=0, concat_axis=2, tiled=True)
    squares = jnp.sum(jnp.square(cache_out.astype(jnp.float32)), axis=2)
    squares = lax.psum(squares, "sub")
    checksum = jnp.sqrt(1.0 + squares / (PAGE * LATENT)).T
    return (cache_out, checksum)


def kept_direct(away):
    return DIRECT if away else MAXP


def most_spilled(pages, n):
    half = n // 2
    full, rest = divmod(min(pages - half, half * MAXP), MAXP)
    return (MAXP - DIRECT) * full + max(0, rest - DIRECT)


def exchange(n, subs, counts_in, tails_in, assign_in, x_in, out, chk, send, tab, part, parts_in,
             send_sem, recv_sem, precv_sem, ready_sem, mate_sem, pair_sem,
             sums, x, counts, tails, assign, spill_sem, relay, spill, *landed):
    me = lax.axis_index("seq")
    sub = lax.axis_index("sub")
    pages, layers, piece = x.shape
    tokens = piece // LATENT
    line = n // ROW_CHIPS
    mid = line // 2
    half = mid * ROW_CHIPS
    spilled = spill.shape[0]
    rest = MAXP - DIRECT
    row = ROW_CHIPS * subs
    z, col = me // ROW_CHIPS, me % ROW_CHIPS
    place_in_row = col * subs + sub
    upper = z // mid
    own_first = upper * half
    far_first = half - own_first
    central = jnp.logical_or(z == mid - 1, z == mid)

    def device(level, spot):
        return {"seq": level * ROW_CHIPS + spot // subs, "sub": spot % subs}

    barrier = pltpu.get_barrier_semaphore()

    def greet(level, spot):
        pl.semaphore_signal(
            barrier, inc=1, device_id=device(level, spot), device_id_type=MESH)

    @pl.when(z == mid)
    def _():
        for spot in range(subs):
            greet(mid - 1, col * subs + spot)

    arrivals = [pltpu.make_async_copy(a, b, send_sem) for a, b in (
        (counts_in, counts), (tails_in, tails), (assign_in, assign), (x_in, x))]
    cuts = math.gcd(pages, 8)
    cut = pages // cuts
    for i in range(cuts):
        part_of = pl.ds(i * cut, cut)
        pltpu.make_async_copy(x_in.at[part_of], x.at[part_of], send_sem).start()
    for copy in arrivals[:3]:
        copy.start()
    for level in range(line):
        @pl.when(z < level)
        def _():
            for spot in range(subs if level == mid else row):
                greet(level, spot + col * subs if level == mid else spot)

    @pl.when(z == mid)
    def _():
        for j in range(1, subs):
            greet(z, col * subs + (sub + j) % subs)

    @pl.when(z != mid)
    def _():
        for j in range(1, row):
            greet(z, (place_in_row + j) % row)

    column = lax.broadcasted_iota(jnp.int32, (layers, piece), 1)
    for f in range(tokens + 1):
        tab[f] = jnp.where(column < f * LATENT, 1.0, 0.0).astype(x.dtype)
    for buffer in landed:
        buffer[spilled] = jnp.zeros((layers, piece), x.dtype)

    for copy in arrivals:
        copy.wait()
    reqs = counts.shape[0]
    packed, begin = [], jnp.int32(0)
    for r in range(reqs):
        packed.append((begin * 16 + counts[r]) * 128 + tails[r])
        begin = begin + counts[r]
    base = (sub * n + me) * tokens

    def request_of(dest):
        info = jnp.int32(0)
        for r in range(reqs):
            info = info + jnp.where(assign[r] == dest, packed[r], 0)
        return info

    ahead = jnp.where(z == mid - 1, half, 0) + jnp.where(central, col, 0)

    def fill(turn):
        dest = (ahead + turn) % n
        info = request_of(dest)
        tail = info & 127
        count = (info >> 7) & 15
        start = info >> 11
        for k in range(MAXP):
            used = k < count
            row_at = jnp.where(used, start + k, 0)
            filled = jnp.where(used, jnp.where(k < count - 1, PAGE, tail), 0)
            keep = jnp.clip(filled - base, 0, tokens)
            send[dest * MAXP + k] = x[row_at] * tab[keep]

    def whole(ref, sem):
        return pltpu.make_async_copy(ref, ref, sem)

    def away_of(level):
        return level - mid if level >= mid else mid - 1 - level

    def spill_starts(first):
        starts, begin = [], jnp.int32(0)
        for j in range(half):
            count = (request_of(first + j) >> 7) & 15
            starts.append((begin, count))
            begin = begin + jnp.maximum(count - DIRECT, 0)
        return starts

    def columns(source, first=0, rows=MAXP):
        return out.at[pl.ds(first, rows), :, pl.ds(pl.multiple_of(source * piece, LANES), piece)]

    def rows_to(zz, level):
        return MAXP if zz // mid == level // mid else kept_direct(away_of(zz))

    def send_piece(zz, level, place):
        dest = level * ROW_CHIPS + place
        rows = rows_to(zz, level)
        pltpu.make_async_remote_copy(
            src_ref=send.at[pl.ds(dest * MAXP, rows)],
            dst_ref=columns(me, 0, rows),
            send_sem=send_sem,
            recv_sem=recv_sem,
            device_id={"seq": dest},
            device_id_type=MESH).start()

    def send_spill(zz):
        away = away_of(zz)
        pltpu.make_async_remote_copy(
            src_ref=spill,
            dst_ref=landed[away - 1].at[pl.ds(0, spilled)],
            send_sem=send_sem,
            recv_sem=spill_sem.at[away - 1],
            device_id={"seq": (mid - 1 if zz >= mid else mid) * ROW_CHIPS + col},
            device_id_type=MESH).start()

    def send_part(level, place):
        pltpu.make_async_remote_copy(
            src_ref=part.at[level * ROW_CHIPS + place],
            dst_ref=parts_in.at[me],
            send_sem=send_sem,
            recv_sem=precv_sem,
            device_id={"seq": level * ROW_CHIPS + place},
            device_id_type=MESH).start()

    def send_parts(level):
        for place in range(ROW_CHIPS):
            send_part(level, place)

    def tell_lower():
        for level in range(line - 1):
            by_entry = jnp.logical_and(level == mid - 1, z == mid)

            @pl.when(jnp.logical_and(level < z, jnp.logical_not(by_entry)))
            def _():
                for spot in range(row):
                    pl.semaphore_signal(
                        ready_sem.at[z - 1], inc=1, device_id=device(level, spot), device_id_type=MESH)

    def send_mate(zz):
        dest = zz * ROW_CHIPS + (col + 1) % ROW_CHIPS
        pltpu.make_async_remote_copy(
            src_ref=send.at[pl.ds(dest * MAXP, MAXP)],
            dst_ref=columns(me),
            send_sem=send_sem,
            recv_sem=recv_sem,
            device_id={"seq": dest},
            device_id_type=MESH).start()

    def forward(away):
        near = spill_starts(own_first)
        level = jnp.where(upper == 1, mid - 1 - away, mid + away)
        source = level * ROW_CHIPS + col
        whole(landed[away - 1].at[pl.ds(0, spilled)], spill_sem.at[away - 1]).wait()
        for j in range(half):
            for k in range(rest):
                at = jnp.where(k + DIRECT < near[j][1], near[j][0] + k, spilled)
                relay[away - 1, j * rest + k] = landed[away - 1][at]
        kept = columns(source, DIRECT, rest)
        for j in range(half):
            @pl.when(own_first + j != me)
            def _():
                pltpu.make_async_remote_copy(
                    src_ref=relay.at[away - 1, pl.ds(j * rest, rest)],
                    dst_ref=kept,
                    send_sem=send_sem,
                    recv_sem=recv_sem,
                    device_id={"seq": own_first + j},
                    device_id_type=MESH).start()
        at_source = pl.ds(pl.multiple_of(source * piece, LANES), piece)
        for k in range(rest):
            out[DIRECT + k, :, at_source] = relay[away - 1, (me - own_first) * rest + k]

    def issue(zz, item):
        if item == SPILL:
            send_spill(zz)
        elif item == RELAY:
            for away in range(mid - 1, 0, -1):
                forward(away)
        elif item // ROW_CHIPS == zz:
            send_mate(zz)
        else:
            send_piece(zz, item // ROW_CHIPS, item % ROW_CHIPS)

    def issue_early(zz):
        for s in range(row):
            @pl.when(jnp.logical_and(z == zz, place_in_row == s))
            def _():
                for item in ORDER[zz][s][:EARLY[zz]]:
                    issue(zz, item)

    def sends_later(zz):
        for level in range(zz):
            send_parts(level)
        if zz != mid:
            send_part(zz, 1 - col)
        if zz == mid - 1:
            send_parts(mid)
        for s in range(row):
            @pl.when(place_in_row == s)
            def _():
                known = zz + 1 if zz == mid - 1 else zz
                for item in ORDER[zz][s][EARLY[zz]:]:
                    target = item // ROW_CHIPS
                    if item == RELAY:
                        target = zz
                    elif item == SPILL:
                        target = mid if zz < mid else 0
                    elif zz == target == mid:
                        target = mid + 1
                    while known < target:
                        known += 1
                        if (zz, known) != (mid - 1, mid):
                            pl.semaphore_wait(ready_sem.at[known - 1], row)
                            send_parts(known)
                            if (zz, known) == (mid, mid + 1):
                                send_part(zz, 1 - col)
                    issue(zz, item)

    def pack_rest():
        for turn in range(2, n):
            fill(turn)

        @pl.when(jnp.logical_not(central))
        def _():
            far = spill_starts(far_first)
            for o in range(spilled):
                at = DIRECT + o
                for j in range(1, half):
                    at = jnp.where(o >= far[j][0], j * MAXP + DIRECT + o - far[j][0], at)
                spill[o] = send[far_first * MAXP + jnp.minimum(at, half * MAXP - 1)]

    for turn in range(2):
        fill(turn)

    @pl.when(jnp.logical_not(central))
    def _():
        pack_rest()

    greeted = z * row + row - 1 + jnp.where(z == mid - 1, subs, 0)
    pl.semaphore_wait(barrier, jnp.where(z == mid, z * subs + subs - 1, greeted))

    for level in (mid - 1, mid):
        issue_early(level)

    @pl.when(z == mid - 1)
    def _():
        for spot in range(subs):
            for level, place in ((mid, col), (mid - 1, 1 - col)):
                pl.semaphore_signal(
                    mate_sem, inc=1, device_id=device(level, place * subs + spot),
                    device_id_type=MESH)

    @pl.when(z != mid)
    def _():
        tell_lower()

    @pl.when(central)
    def _():
        pack_rest()
    for level in range(line):
        if level not in (mid - 1, mid):
            issue_early(level)

    lane = lax.broadcasted_iota(jnp.int32, (layers, LANES), 1)
    for dest in range(n):
        total = jnp.zeros((layers, LANES), jnp.float32)
        for k in range(MAXP):
            v = send[dest * MAXP + k].astype(jnp.float32)
            s = jnp.sum(v * v, axis=1, keepdims=True)
            total = jnp.where(lane == k, s, total)
        part[dest] = total
    mine = pl.ds(pl.multiple_of(me * piece, LANES), piece)
    for k in range(MAXP):
        out[k, :, mine] = send[me * MAXP + k]
    parts_in[me] = part[me]

    @pl.when(central)
    def _():
        pl.semaphore_wait(mate_sem, subs)

    @pl.when(z == mid)
    def _():
        tell_lower()

    for level in range(line):
        @pl.when(z == level)
        def _():
            sends_later(level)

    whole(parts_in.at[pl.ds(0, n - 1)], precv_sem).wait()
    sums[0] = jnp.sum(parts_in[...], axis=0)
    pair = pltpu.make_async_remote_copy(
        src_ref=sums.at[0],
        dst_ref=sums.at[1],
        send_sem=send_sem,
        recv_sem=pair_sem,
        device_id={"sub": 1 - sub},
        device_id_type=MESH)
    pair.start()
    pair.wait_recv()
    total = sums[0] + sums[1]
    chk[...] = jnp.sqrt(1.0 + total / (PAGE * LATENT))[:, :MAXP]
    whole(parts_in, send_sem).wait()
    for level in range(line):
        away = away_of(level)
        forwards = 0 if away else mid - 1
        sent = (half - 1) * MAXP + half * kept_direct(away)
        got = (n - 1) * MAXP - forwards * rest

        @pl.when(z == level)
        def _():
            whole(send.at[pl.ds(0, sent)], send_sem).wait()
            if away:
                whole(spill, send_sem).wait()
            else:
                whole(send.at[pl.ds(0, forwards * (half - 1) * rest)], send_sem).wait()
            whole(send.at[pl.ds(0, got)], recv_sem).wait()


def place(pages_in, sums_in, pages, sums, sem):
    copies = [pltpu.make_async_copy(a, b, sem.at[k]) for k, (a, b) in enumerate(
        ((pages_in, pages), (sums_in, sums)))]
    for copy in copies:
        copy.start()
    for copy in copies:
        copy.wait()


def direct(cache_in, page_counts, tail_tokens, assignment):
    n, subs = lax.axis_size("seq"), lax.axis_size("sub")
    pages, layers, piece = cache_in.shape
    mid = n // ROW_CHIPS // 2
    spilled = most_spilled(pages, n)
    vmem = pl.BlockSpec(memory_space=pltpu.VMEM)
    landed = pl.pallas_call(
        functools.partial(exchange, n, subs),
        out_shape=(pltpu.VMEM((MAXP, layers, piece * n), cache_in.dtype),
                   pltpu.VMEM((layers, MAXP), jnp.float32)),
        in_specs=[pl.BlockSpec(memory_space=pl.ANY)] * 4,
        out_specs=(vmem, vmem),
        scratch_shapes=[
            pltpu.VMEM((n * MAXP, layers, piece), cache_in.dtype),
            pltpu.VMEM((piece // LATENT + 1, layers, piece), cache_in.dtype),
            pltpu.VMEM((n, layers, LANES), jnp.float32),
            pltpu.VMEM((n, layers, LANES), jnp.float32),
            pltpu.SemaphoreType.DMA,
            pltpu.SemaphoreType.DMA,
            pltpu.SemaphoreType.DMA,
            pltpu.SemaphoreType.REGULAR((n // ROW_CHIPS - 1,)),
            pltpu.SemaphoreType.REGULAR,
            pltpu.SemaphoreType.DMA,
            pltpu.VMEM((2, layers, LANES), jnp.float32),
            pltpu.VMEM(cache_in.shape, cache_in.dtype),
            pltpu.SMEM(page_counts.shape, jnp.int32),
            pltpu.SMEM(page_counts.shape, jnp.int32),
            pltpu.SMEM(page_counts.shape, jnp.int32),
            pltpu.SemaphoreType.DMA((mid - 1,)),
            pltpu.VMEM((mid - 1, n // 2 * (MAXP - DIRECT), layers, piece), cache_in.dtype),
            pltpu.VMEM((spilled, layers, piece), cache_in.dtype),
        ] + [pltpu.VMEM((spilled + 1, layers, piece), cache_in.dtype)] * (mid - 1),
        compiler_params=pltpu.CompilerParams(collective_id=0, has_side_effects=True),
    )(page_counts, tail_tokens, assignment, cache_in)
    return pl.pallas_call(
        place,
        out_shape=tuple(jax.ShapeDtypeStruct(a.shape, a.dtype) for a in landed),
        in_specs=[vmem] * 2,
        out_specs=(pl.BlockSpec(memory_space=pltpu.HBM),) * 2,
        scratch_shapes=[pltpu.SemaphoreType.DMA((2,))],
    )(*(pltpu.with_memory_space_constraint(a, pltpu.VMEM) for a in landed))


def shards(cache_in, page_counts, tail_tokens, assignment):
    pages, _, piece = cache_in.shape
    n, subs = lax.axis_size("seq"), lax.axis_size("sub")
    whole_tiles = piece % LANES == 0 and piece % LATENT == 0
    in_order = n == len(ORDER) * ROW_CHIPS and subs == 2 and subs * ROW_CHIPS == len(ORDER[0])
    fits = in_order and page_counts.shape[0] == n
    return (direct if whole_tiles and fits else general)(cache_in, page_counts, tail_tokens, assignment)


def solution(mesh):
    placed = (P("groups", None, ("sub", "seq")), P("groups"), P("groups"), P("groups"))
    return jax.shard_map(
        shards,
        mesh=mesh,
        in_specs=placed,
        out_specs=(P(("groups", "seq"), None, "sub"), P(None, ("groups", "seq"))),
        check_vma=False,
    )
```

```python
import functools
import math

import jax
import jax.numpy as jnp
from jax import lax
from jax.experimental import pallas as pl
from jax.experimental.pallas import tpu as pltpu
from jax.sharding import PartitionSpec as P

LATENT = 576
PAGE = 64
MAXP = 8
LANES = 128
ROW_CHIPS = 2
DIRECT = 4
SPILL, RELAY = 8, 9
ORDER = [
    [[1, 3, 8, 7, 6, 2, 5, 4], [1, 2, 8, 7, 6, 3, 5, 4], [0, 2, 8, 6, 7, 3, 4, 5], [0, 3, 8, 6, 7, 2, 4, 5]],
    [[4, 5, 3, 0, 7, 6, 9, 1], [4, 5, 3, 0, 7, 6, 9, 1], [5, 4, 2, 0, 6, 7, 9, 1], [5, 4, 2, 0, 6, 7, 9, 1]],
    [[0, 1, 3, 2, 7, 6, 5, 9], [0, 1, 3, 2, 6, 7, 5, 9], [1, 0, 2, 3, 6, 7, 4, 9], [1, 0, 2, 3, 7, 6, 4, 9]],
    [[8, 0, 1, 7, 5, 4, 3, 2], [8, 0, 1, 7, 4, 5, 2, 3], [8, 0, 1, 6, 4, 5, 2, 3], [8, 0, 1, 6, 5, 4, 3, 2]],
]
EARLY = [0, 1, 1, 1]
MESH = pl.DeviceIdType.MESH


def by_device(matches, values):
    return jnp.sum(jnp.where(matches, values[None, :], 0), axis=1)


def general(cache_in, page_counts, tail_tokens, assignment):
    seq_count = lax.axis_size("seq")
    own_index = lax.axis_index("seq")
    sub_index = lax.axis_index("sub")
    total_pages, layer_count, piece = cache_in.shape
    starts = jnp.cumsum(page_counts) - page_counts
    device_ids = jnp.arange(seq_count, dtype=jnp.int32)
    matches = assignment[None, :] == device_ids[:, None]
    dest_counts = by_device(matches, page_counts)
    dest_starts = by_device(matches, starts)
    dest_tails = by_device(matches, tail_tokens)
    slot_ids = jnp.arange(seq_count * MAXP, dtype=jnp.int32)
    page_rank = slot_ids % MAXP
    counts_at = jnp.repeat(dest_counts, MAXP)
    starts_at = jnp.repeat(dest_starts, MAXP)
    tails_at = jnp.repeat(dest_tails, MAXP)
    in_use = page_rank < counts_at
    source_rows = jnp.where(in_use, starts_at + page_rank, 0)
    filled = jnp.where(in_use, jnp.where(page_rank < counts_at - 1, PAGE, tails_at), 0)
    column = (sub_index * seq_count + own_index) * piece + jnp.arange(piece, dtype=jnp.int32)
    token_of = column // LATENT
    kept_mask = token_of[None, :] < filled[:, None]
    zero_value = jnp.zeros((), cache_in.dtype)
    fetched = jnp.take(cache_in, source_rows, axis=0)
    packed = jnp.where(kept_mask[:, None, :], fetched, zero_value)
    cache_out = lax.all_to_all(packed, "seq", split_axis=0, concat_axis=2, tiled=True)
    squares = jnp.sum(jnp.square(cache_out.astype(jnp.float32)), axis=2)
    squares = lax.psum(squares, "sub")
    checksum = jnp.sqrt(1.0 + squares / (PAGE * LATENT)).T
    return (cache_out, checksum)


def kept_direct(away):
    return DIRECT if away else MAXP


def most_spilled(pages, n):
    half = n // 2
    full, rest = divmod(min(pages - half, half * MAXP), MAXP)
    return (MAXP - DIRECT) * full + max(0, rest - DIRECT)


def exchange(n, subs, counts_in, tails_in, assign_in, x_in, out, chk, send, tab, part, parts_in,
             send_sem, recv_sem, precv_sem, ready_sem, mate_sem, pair_sem, in_sem,
             sums, x, counts, tails, assign, spill_sem, relay, spill, *landed):
    me = lax.axis_index("seq")
    sub = lax.axis_index("sub")
    pages, layers, piece = x.shape
    tokens = piece // LATENT
    line = n // ROW_CHIPS
    mid = line // 2
    half = mid * ROW_CHIPS
    spilled = spill.shape[0]
    rest = MAXP - DIRECT
    row = ROW_CHIPS * subs
    z, col = me // ROW_CHIPS, me % ROW_CHIPS
    place_in_row = col * subs + sub
    upper = z // mid
    own_first = upper * half
    far_first = half - own_first
    central = jnp.logical_or(z == mid - 1, z == mid)

    def device(level, spot):
        return {"seq": level * ROW_CHIPS + spot // subs, "sub": spot % subs}

    barrier = pltpu.get_barrier_semaphore()

    def greet(level, spot):
        pl.semaphore_signal(
            barrier, inc=1, device_id=device(level, spot), device_id_type=MESH)

    @pl.when(z == mid)
    def _():
        for spot in range(subs):
            greet(mid - 1, col * subs + spot)

    arrivals = [pltpu.make_async_copy(a, b, send_sem) for a, b in (
        (counts_in, counts), (tails_in, tails), (assign_in, assign))]
    pages_here = pltpu.make_async_copy(x_in, x, in_sem)
    cuts = math.gcd(pages, 8)
    cut = pages // cuts
    for i in range(cuts):
        part_of = pl.ds(i * cut, cut)
        pltpu.make_async_copy(x_in.at[part_of], x.at[part_of], in_sem).start()
    for copy in arrivals:
        copy.start()
    for level in range(line):
        @pl.when(z < level)
        def _():
            for spot in range(subs if level == mid else row):
                greet(level, spot + col * subs if level == mid else spot)

    @pl.when(z == mid)
    def _():
        for j in range(1, subs):
            greet(z, col * subs + (sub + j) % subs)

    @pl.when(z != mid)
    def _():
        for j in range(1, row):
            greet(z, (place_in_row + j) % row)

    column = lax.broadcasted_iota(jnp.int32, (layers, piece), 1)
    for f in range(tokens + 1):
        tab[f] = jnp.where(column < f * LATENT, 1.0, 0.0).astype(x.dtype)
    for buffer in landed:
        buffer[spilled] = jnp.zeros((layers, piece), x.dtype)

    for copy in arrivals:
        copy.wait()
    reqs = counts.shape[0]
    packed, begin = [], jnp.int32(0)
    for r in range(reqs):
        packed.append((begin * 16 + counts[r]) * 128 + tails[r])
        begin = begin + counts[r]
    base = (sub * n + me) * tokens

    def request_of(dest):
        info = jnp.int32(0)
        for r in range(reqs):
            info = info + jnp.where(assign[r] == dest, packed[r], 0)
        return info

    ahead = jnp.where(z == mid - 1, half, 0) + jnp.where(central, col, 0)

    first_two = [request_of((ahead + turn) % n) for turn in range(2)]
    pages_here.wait()

    def fill(turn):
        dest = (ahead + turn) % n
        info = first_two[turn] if turn < 2 else request_of(dest)
        tail = info & 127
        count = (info >> 7) & 15
        start = info >> 11
        for k in range(MAXP):
            used = k < count
            row_at = jnp.where(used, start + k, 0)
            filled = jnp.where(used, jnp.where(k < count - 1, PAGE, tail), 0)
            keep = jnp.clip(filled - base, 0, tokens)
            send[dest * MAXP + k] = x[row_at] * tab[keep]

    def whole(ref, sem):
        return pltpu.make_async_copy(ref, ref, sem)

    def away_of(level):
        return level - mid if level >= mid else mid - 1 - level

    def spill_starts(first):
        starts, begin = [], jnp.int32(0)
        for j in range(half):
            count = (request_of(first + j) >> 7) & 15
            starts.append((begin, count))
            begin = begin + jnp.maximum(count - DIRECT, 0)
        return starts

    def columns(source, first=0, rows=MAXP):
        return out.at[pl.ds(first, rows), :, pl.ds(pl.multiple_of(source * piece, LANES), piece)]

    def rows_to(zz, level):
        return MAXP if zz // mid == level // mid else kept_direct(away_of(zz))

    def send_piece(zz, level, place):
        dest = level * ROW_CHIPS + place
        rows = rows_to(zz, level)
        pltpu.make_async_remote_copy(
            src_ref=send.at[pl.ds(dest * MAXP, rows)],
            dst_ref=columns(me, 0, rows),
            send_sem=send_sem,
            recv_sem=recv_sem,
            device_id={"seq": dest},
            device_id_type=MESH).start()

    def send_spill(zz):
        away = away_of(zz)
        pltpu.make_async_remote_copy(
            src_ref=spill,
            dst_ref=landed[away - 1].at[pl.ds(0, spilled)],
            send_sem=send_sem,
            recv_sem=spill_sem.at[away - 1],
            device_id={"seq": (mid - 1 if zz >= mid else mid) * ROW_CHIPS + col},
            device_id_type=MESH).start()

    def send_part(level, place):
        pltpu.make_async_remote_copy(
            src_ref=part.at[level * ROW_CHIPS + place],
            dst_ref=parts_in.at[me],
            send_sem=send_sem,
            recv_sem=precv_sem,
            device_id={"seq": level * ROW_CHIPS + place},
            device_id_type=MESH).start()

    def send_parts(level):
        for place in range(ROW_CHIPS):
            send_part(level, place)

    def tell_lower():
        for level in range(line - 1):
            by_entry = jnp.logical_and(level == mid - 1, z == mid)

            @pl.when(jnp.logical_and(level < z, jnp.logical_not(by_entry)))
            def _():
                for spot in range(row):
                    pl.semaphore_signal(
                        ready_sem.at[z - 1], inc=1, device_id=device(level, spot), device_id_type=MESH)

    def send_mate(zz):
        dest = zz * ROW_CHIPS + (col + 1) % ROW_CHIPS
        pltpu.make_async_remote_copy(
            src_ref=send.at[pl.ds(dest * MAXP, MAXP)],
            dst_ref=columns(me),
            send_sem=send_sem,
            recv_sem=recv_sem,
            device_id={"seq": dest},
            device_id_type=MESH).start()

    def forward(away):
        near = spill_starts(own_first)
        level = jnp.where(upper == 1, mid - 1 - away, mid + away)
        source = level * ROW_CHIPS + col
        whole(landed[away - 1].at[pl.ds(0, spilled)], spill_sem.at[away - 1]).wait()
        for j in range(half):
            for k in range(rest):
                at = jnp.where(k + DIRECT < near[j][1], near[j][0] + k, spilled)
                relay[away - 1, j * rest + k] = landed[away - 1][at]
        kept = columns(source, DIRECT, rest)
        for j in range(half):
            @pl.when(own_first + j != me)
            def _():
                pltpu.make_async_remote_copy(
                    src_ref=relay.at[away - 1, pl.ds(j * rest, rest)],
                    dst_ref=kept,
                    send_sem=send_sem,
                    recv_sem=recv_sem,
                    device_id={"seq": own_first + j},
                    device_id_type=MESH).start()
        at_source = pl.ds(pl.multiple_of(source * piece, LANES), piece)
        for k in range(rest):
            out[DIRECT + k, :, at_source] = relay[away - 1, (me - own_first) * rest + k]

    def issue(zz, item):
        if item == SPILL:
            send_spill(zz)
        elif item == RELAY:
            for away in range(mid - 1, 0, -1):
                forward(away)
        elif item // ROW_CHIPS == zz:
            send_mate(zz)
        else:
            send_piece(zz, item // ROW_CHIPS, item % ROW_CHIPS)

    def issue_early(zz):
        for s in range(row):
            @pl.when(jnp.logical_and(z == zz, place_in_row == s))
            def _():
                for item in ORDER[zz][s][:EARLY[zz]]:
                    issue(zz, item)

    def sends_later(zz):
        for level in range(zz):
            send_parts(level)
        if zz != mid:
            send_part(zz, 1 - col)
        if zz == mid - 1:
            send_parts(mid)
        for s in range(row):
            @pl.when(place_in_row == s)
            def _():
                known = zz + 1 if zz == mid - 1 else zz
                for item in ORDER[zz][s][EARLY[zz]:]:
                    target = item // ROW_CHIPS
                    if item == RELAY:
                        target = zz
                    elif item == SPILL:
                        target = mid if zz < mid else 0
                    elif zz == target == mid:
                        target = mid + 1
                    while known < target:
                        known += 1
                        if (zz, known) != (mid - 1, mid):
                            pl.semaphore_wait(ready_sem.at[known - 1], row)
                            send_parts(known)
                            if (zz, known) == (mid, mid + 1):
                                send_part(zz, 1 - col)
                    issue(zz, item)

    def pack_rest():
        for turn in range(2, n):
            fill(turn)

        @pl.when(jnp.logical_not(central))
        def _():
            far = spill_starts(far_first)
            for o in range(spilled):
                at = DIRECT + o
                for j in range(1, half):
                    at = jnp.where(o >= far[j][0], j * MAXP + DIRECT + o - far[j][0], at)
                spill[o] = send[far_first * MAXP + jnp.minimum(at, half * MAXP - 1)]

    for turn in range(2):
        fill(turn)

    @pl.when(jnp.logical_not(central))
    def _():
        pack_rest()

    greeted = z * row + row - 1 + jnp.where(z == mid - 1, subs, 0)
    pl.semaphore_wait(barrier, jnp.where(z == mid, z * subs + subs - 1, greeted))

    for level in (mid - 1, mid):
        issue_early(level)

    @pl.when(z == mid - 1)
    def _():
        for spot in range(subs):
            for level, place in ((mid, col), (mid - 1, 1 - col)):
                pl.semaphore_signal(
                    mate_sem, inc=1, device_id=device(level, place * subs + spot),
                    device_id_type=MESH)

    @pl.when(z != mid)
    def _():
        tell_lower()

    @pl.when(central)
    def _():
        pack_rest()
    for level in range(line):
        if level not in (mid - 1, mid):
            issue_early(level)

    lane = lax.broadcasted_iota(jnp.int32, (layers, LANES), 1)
    for dest in range(n):
        total = jnp.zeros((layers, LANES), jnp.float32)
        for k in range(MAXP):
            v = send[dest * MAXP + k].astype(jnp.float32)
            s = jnp.sum(v * v, axis=1, keepdims=True)
            total = jnp.where(lane == k, s, total)
        part[dest] = total
    mine = pl.ds(pl.multiple_of(me * piece, LANES), piece)
    for k in range(MAXP):
        out[k, :, mine] = send[me * MAXP + k]
    parts_in[me] = part[me]

    @pl.when(central)
    def _():
        pl.semaphore_wait(mate_sem, subs)

    @pl.when(z == mid)
    def _():
        tell_lower()

    for level in range(line):
        @pl.when(z == level)
        def _():
            sends_later(level)

    whole(parts_in.at[pl.ds(0, n - 1)], precv_sem).wait()
    sums[0] = jnp.sum(parts_in[...], axis=0)
    pair = pltpu.make_async_remote_copy(
        src_ref=sums.at[0],
        dst_ref=sums.at[1],
        send_sem=send_sem,
        recv_sem=pair_sem,
        device_id={"sub": 1 - sub},
        device_id_type=MESH)
    pair.start()
    pair.wait_recv()
    total = sums[0] + sums[1]
    chk[...] = jnp.sqrt(1.0 + total / (PAGE * LATENT))[:, :MAXP]
    whole(parts_in, send_sem).wait()
    for level in range(line):
        away = away_of(level)
        forwards = 0 if away else mid - 1
        sent = (half - 1) * MAXP + half * kept_direct(away)
        got = (n - 1) * MAXP - forwards * rest

        @pl.when(z == level)
        def _():
            whole(send.at[pl.ds(0, sent)], send_sem).wait()
            if away:
                whole(spill, send_sem).wait()
            else:
                whole(send.at[pl.ds(0, forwards * (half - 1) * rest)], send_sem).wait()
            whole(send.at[pl.ds(0, got)], recv_sem).wait()


def place(pages_in, sums_in, pages, sums, sem):
    copies = [pltpu.make_async_copy(a, b, sem.at[k]) for k, (a, b) in enumerate(
        ((pages_in, pages), (sums_in, sums)))]
    for copy in copies:
        copy.start()
    for copy in copies:
        copy.wait()


def direct(cache_in, page_counts, tail_tokens, assignment):
    n, subs = lax.axis_size("seq"), lax.axis_size("sub")
    pages, layers, piece = cache_in.shape
    mid = n // ROW_CHIPS // 2
    spilled = most_spilled(pages, n)
    vmem = pl.BlockSpec(memory_space=pltpu.VMEM)
    landed = pl.pallas_call(
        functools.partial(exchange, n, subs),
        out_shape=(pltpu.VMEM((MAXP, layers, piece * n), cache_in.dtype),
                   pltpu.VMEM((layers, MAXP), jnp.float32)),
        in_specs=[pl.BlockSpec(memory_space=pl.ANY)] * 4,
        out_specs=(vmem, vmem),
        scratch_shapes=[
            pltpu.VMEM((n * MAXP, layers, piece), cache_in.dtype),
            pltpu.VMEM((piece // LATENT + 1, layers, piece), cache_in.dtype),
            pltpu.VMEM((n, layers, LANES), jnp.float32),
            pltpu.VMEM((n, layers, LANES), jnp.float32),
            pltpu.SemaphoreType.DMA,
            pltpu.SemaphoreType.DMA,
            pltpu.SemaphoreType.DMA,
            pltpu.SemaphoreType.REGULAR((n // ROW_CHIPS - 1,)),
            pltpu.SemaphoreType.REGULAR,
            pltpu.SemaphoreType.DMA,
            pltpu.SemaphoreType.DMA,
            pltpu.VMEM((2, layers, LANES), jnp.float32),
            pltpu.VMEM(cache_in.shape, cache_in.dtype),
            pltpu.SMEM(page_counts.shape, jnp.int32),
            pltpu.SMEM(page_counts.shape, jnp.int32),
            pltpu.SMEM(page_counts.shape, jnp.int32),
            pltpu.SemaphoreType.DMA((mid - 1,)),
            pltpu.VMEM((mid - 1, n // 2 * (MAXP - DIRECT), layers, piece), cache_in.dtype),
            pltpu.VMEM((spilled, layers, piece), cache_in.dtype),
        ] + [pltpu.VMEM((spilled + 1, layers, piece), cache_in.dtype)] * (mid - 1),
        compiler_params=pltpu.CompilerParams(collective_id=0, has_side_effects=True),
    )(page_counts, tail_tokens, assignment, cache_in)
    return pl.pallas_call(
        place,
        out_shape=tuple(jax.ShapeDtypeStruct(a.shape, a.dtype) for a in landed),
        in_specs=[vmem] * 2,
        out_specs=(pl.BlockSpec(memory_space=pltpu.HBM),) * 2,
        scratch_shapes=[pltpu.SemaphoreType.DMA((2,))],
    )(*(pltpu.with_memory_space_constraint(a, pltpu.VMEM) for a in landed))


def shards(cache_in, page_counts, tail_tokens, assignment):
    pages, _, piece = cache_in.shape
    n, subs = lax.axis_size("seq"), lax.axis_size("sub")
    whole_tiles = piece % LANES == 0 and piece % LATENT == 0
    in_order = n == len(ORDER) * ROW_CHIPS and subs == 2 and subs * ROW_CHIPS == len(ORDER[0])
    fits = in_order and page_counts.shape[0] == n
    return (direct if whole_tiles and fits else general)(cache_in, page_counts, tail_tokens, assignment)


def solution(mesh):
    placed = (P("groups", None, ("sub", "seq")), P("groups"), P("groups"), P("groups"))
    return jax.shard_map(
        shards,
        mesh=mesh,
        in_specs=placed,
        out_specs=(P(("groups", "seq"), None, "sub"), P(None, ("groups", "seq"))),
        check_vma=False,
    )
```

```python
import functools
import math

import jax
import jax.numpy as jnp
from jax import lax
from jax.experimental import pallas as pl
from jax.experimental.pallas import tpu as pltpu
from jax.sharding import PartitionSpec as P

LATENT = 576
PAGE = 64
MAXP = 8
LANES = 128
ROW_CHIPS = 2
DIRECT = 4
SPILL, RELAY = 8, 9
ORDER = [
    [[1, 3, 8, 7, 6, 2, 5, 4], [1, 2, 8, 7, 6, 3, 5, 4], [0, 2, 8, 6, 7, 3, 4, 5], [0, 3, 8, 6, 7, 2, 4, 5]],
    [[4, 5, 3, 0, 7, 6, 9, 1], [4, 5, 3, 0, 7, 6, 9, 1], [5, 4, 2, 0, 6, 7, 9, 1], [5, 4, 2, 0, 6, 7, 9, 1]],
    [[0, 1, 3, 2, 7, 6, 5, 9], [0, 1, 3, 2, 6, 7, 5, 9], [1, 0, 2, 3, 6, 7, 4, 9], [1, 0, 2, 3, 7, 6, 4, 9]],
    [[8, 0, 1, 7, 5, 4, 3, 2], [8, 0, 1, 7, 4, 5, 2, 3], [8, 0, 1, 6, 4, 5, 2, 3], [8, 0, 1, 6, 5, 4, 3, 2]],
]
EARLY = [0, 1, 1, 3]
MESH = pl.DeviceIdType.MESH


def by_device(matches, values):
    return jnp.sum(jnp.where(matches, values[None, :], 0), axis=1)


def general(cache_in, page_counts, tail_tokens, assignment):
    seq_count = lax.axis_size("seq")
    own_index = lax.axis_index("seq")
    sub_index = lax.axis_index("sub")
    total_pages, layer_count, piece = cache_in.shape
    starts = jnp.cumsum(page_counts) - page_counts
    device_ids = jnp.arange(seq_count, dtype=jnp.int32)
    matches = assignment[None, :] == device_ids[:, None]
    dest_counts = by_device(matches, page_counts)
    dest_starts = by_device(matches, starts)
    dest_tails = by_device(matches, tail_tokens)
    slot_ids = jnp.arange(seq_count * MAXP, dtype=jnp.int32)
    page_rank = slot_ids % MAXP
    counts_at = jnp.repeat(dest_counts, MAXP)
    starts_at = jnp.repeat(dest_starts, MAXP)
    tails_at = jnp.repeat(dest_tails, MAXP)
    in_use = page_rank < counts_at
    source_rows = jnp.where(in_use, starts_at + page_rank, 0)
    filled = jnp.where(in_use, jnp.where(page_rank < counts_at - 1, PAGE, tails_at), 0)
    column = (sub_index * seq_count + own_index) * piece + jnp.arange(piece, dtype=jnp.int32)
    token_of = column // LATENT
    kept_mask = token_of[None, :] < filled[:, None]
    zero_value = jnp.zeros((), cache_in.dtype)
    fetched = jnp.take(cache_in, source_rows, axis=0)
    packed = jnp.where(kept_mask[:, None, :], fetched, zero_value)
    cache_out = lax.all_to_all(packed, "seq", split_axis=0, concat_axis=2, tiled=True)
    squares = jnp.sum(jnp.square(cache_out.astype(jnp.float32)), axis=2)
    squares = lax.psum(squares, "sub")
    checksum = jnp.sqrt(1.0 + squares / (PAGE * LATENT)).T
    return (cache_out, checksum)


def kept_direct(away):
    return DIRECT if away else MAXP


def most_spilled(pages, n):
    half = n // 2
    full, rest = divmod(min(pages - half, half * MAXP), MAXP)
    return (MAXP - DIRECT) * full + max(0, rest - DIRECT)


def exchange(n, subs, counts_in, tails_in, assign_in, x_in, out, chk, send, tab, part, parts_in,
             send_sem, recv_sem, precv_sem, ready_sem, mate_sem, pair_sem,
             sums, x, counts, tails, assign, spill_sem, relay, spill, *landed):
    me = lax.axis_index("seq")
    sub = lax.axis_index("sub")
    pages, layers, piece = x.shape
    tokens = piece // LATENT
    line = n // ROW_CHIPS
    mid = line // 2
    half = mid * ROW_CHIPS
    spilled = spill.shape[0]
    rest = MAXP - DIRECT
    row = ROW_CHIPS * subs
    z, col = me // ROW_CHIPS, me % ROW_CHIPS
    place_in_row = col * subs + sub
    upper = z // mid
    own_first = upper * half
    far_first = half - own_first
    central = jnp.logical_or(z == mid - 1, z == mid)

    def device(level, spot):
        return {"seq": level * ROW_CHIPS + spot // subs, "sub": spot % subs}

    barrier = pltpu.get_barrier_semaphore()

    def greet(level, spot):
        pl.semaphore_signal(
            barrier, inc=1, device_id=device(level, spot), device_id_type=MESH)

    @pl.when(z == mid)
    def _():
        for spot in range(subs):
            greet(mid - 1, col * subs + spot)

    arrivals = [pltpu.make_async_copy(a, b, send_sem) for a, b in (
        (counts_in, counts), (tails_in, tails), (assign_in, assign), (x_in, x))]
    cuts = math.gcd(pages, 8)
    cut = pages // cuts
    for i in range(cuts):
        part_of = pl.ds(i * cut, cut)
        pltpu.make_async_copy(x_in.at[part_of], x.at[part_of], send_sem).start()
    for copy in arrivals[:3]:
        copy.start()
    for level in range(line):
        @pl.when(z < level)
        def _():
            for spot in range(subs if level == mid else row):
                greet(level, spot + col * subs if level == mid else spot)

    @pl.when(z == mid)
    def _():
        for j in range(1, subs):
            greet(z, col * subs + (sub + j) % subs)

    @pl.when(z != mid)
    def _():
        for j in range(1, row):
            greet(z, (place_in_row + j) % row)

    column = lax.broadcasted_iota(jnp.int32, (layers, piece), 1)
    for f in range(tokens + 1):
        tab[f] = jnp.where(column < f * LATENT, 1.0, 0.0).astype(x.dtype)
    for buffer in landed:
        buffer[spilled] = jnp.zeros((layers, piece), x.dtype)

    for copy in arrivals:
        copy.wait()
    reqs = counts.shape[0]
    packed, begin = [], jnp.int32(0)
    for r in range(reqs):
        packed.append((begin * 16 + counts[r]) * 128 + tails[r])
        begin = begin + counts[r]
    base = (sub * n + me) * tokens

    def request_of(dest):
        info = jnp.int32(0)
        for r in range(reqs):
            info = info + jnp.where(assign[r] == dest, packed[r], 0)
        return info

    ahead = jnp.where(z == mid - 1, half, 0) + jnp.where(central, col, 0)

    def fill(turn):
        dest = (ahead + turn) % n
        info = request_of(dest)
        tail = info & 127
        count = (info >> 7) & 15
        start = info >> 11
        for k in range(MAXP):
            used = k < count
            row_at = jnp.where(used, start + k, 0)
            filled = jnp.where(used, jnp.where(k < count - 1, PAGE, tail), 0)
            keep = jnp.clip(filled - base, 0, tokens)
            send[dest * MAXP + k] = x[row_at] * tab[keep]

    def whole(ref, sem):
        return pltpu.make_async_copy(ref, ref, sem)

    def away_of(level):
        return level - mid if level >= mid else mid - 1 - level

    def spill_starts(first):
        starts, begin = [], jnp.int32(0)
        for j in range(half):
            count = (request_of(first + j) >> 7) & 15
            starts.append((begin, count))
            begin = begin + jnp.maximum(count - DIRECT, 0)
        return starts

    def columns(source, first=0, rows=MAXP):
        return out.at[pl.ds(first, rows), :, pl.ds(pl.multiple_of(source * piece, LANES), piece)]

    def rows_to(zz, level):
        return MAXP if zz // mid == level // mid else kept_direct(away_of(zz))

    def send_piece(zz, level, place):
        dest = level * ROW_CHIPS + place
        rows = rows_to(zz, level)
        pltpu.make_async_remote_copy(
            src_ref=send.at[pl.ds(dest * MAXP, rows)],
            dst_ref=columns(me, 0, rows),
            send_sem=send_sem,
            recv_sem=recv_sem,
            device_id={"seq": dest},
            device_id_type=MESH).start()

    def send_spill(zz):
        away = away_of(zz)
        pltpu.make_async_remote_copy(
            src_ref=spill,
            dst_ref=landed[away - 1].at[pl.ds(0, spilled)],
            send_sem=send_sem,
            recv_sem=spill_sem.at[away - 1],
            device_id={"seq": (mid - 1 if zz >= mid else mid) * ROW_CHIPS + col},
            device_id_type=MESH).start()

    def send_part(level, place):
        pltpu.make_async_remote_copy(
            src_ref=part.at[level * ROW_CHIPS + place],
            dst_ref=parts_in.at[me],
            send_sem=send_sem,
            recv_sem=precv_sem,
            device_id={"seq": level * ROW_CHIPS + place},
            device_id_type=MESH).start()

    def send_parts(level):
        for place in range(ROW_CHIPS):
            send_part(level, place)

    def tell_lower():
        for level in range(line - 1):
            by_entry = jnp.logical_and(level == mid - 1, z == mid)

            @pl.when(jnp.logical_and(level < z, jnp.logical_not(by_entry)))
            def _():
                for spot in range(row):
                    pl.semaphore_signal(
                        ready_sem.at[z - 1], inc=1, device_id=device(level, spot), device_id_type=MESH)

    def send_mate(zz):
        dest = zz * ROW_CHIPS + (col + 1) % ROW_CHIPS
        pltpu.make_async_remote_copy(
            src_ref=send.at[pl.ds(dest * MAXP, MAXP)],
            dst_ref=columns(me),
            send_sem=send_sem,
            recv_sem=recv_sem,
            device_id={"seq": dest},
            device_id_type=MESH).start()

    def forward(away):
        near = spill_starts(own_first)
        level = jnp.where(upper == 1, mid - 1 - away, mid + away)
        source = level * ROW_CHIPS + col
        whole(landed[away - 1].at[pl.ds(0, spilled)], spill_sem.at[away - 1]).wait()
        for j in range(half):
            for k in range(rest):
                at = jnp.where(k + DIRECT < near[j][1], near[j][0] + k, spilled)
                relay[away - 1, j * rest + k] = landed[away - 1][at]
        kept = columns(source, DIRECT, rest)
        for j in range(half):
            @pl.when(own_first + j != me)
            def _():
                pltpu.make_async_remote_copy(
                    src_ref=relay.at[away - 1, pl.ds(j * rest, rest)],
                    dst_ref=kept,
                    send_sem=send_sem,
                    recv_sem=recv_sem,
                    device_id={"seq": own_first + j},
                    device_id_type=MESH).start()
        at_source = pl.ds(pl.multiple_of(source * piece, LANES), piece)
        for k in range(rest):
            out[DIRECT + k, :, at_source] = relay[away - 1, (me - own_first) * rest + k]

    def issue(zz, item):
        if item == SPILL:
            send_spill(zz)
        elif item == RELAY:
            for away in range(mid - 1, 0, -1):
                forward(away)
        elif item // ROW_CHIPS == zz:
            send_mate(zz)
        else:
            send_piece(zz, item // ROW_CHIPS, item % ROW_CHIPS)

    def issue_early(zz):
        for s in range(row):
            @pl.when(jnp.logical_and(z == zz, place_in_row == s))
            def _():
                for item in ORDER[zz][s][:EARLY[zz]]:
                    issue(zz, item)

    def sends_later(zz):
        for level in range(zz):
            send_parts(level)
        if zz != mid:
            send_part(zz, 1 - col)
        if zz == mid - 1:
            send_parts(mid)
        for s in range(row):
            @pl.when(place_in_row == s)
            def _():
                known = zz + 1 if zz == mid - 1 else zz
                for item in ORDER[zz][s][EARLY[zz]:]:
                    target = item // ROW_CHIPS
                    if item == RELAY:
                        target = zz
                    elif item == SPILL:
                        target = mid if zz < mid else 0
                    elif zz == target == mid:
                        target = mid + 1
                    while known < target:
                        known += 1
                        if (zz, known) != (mid - 1, mid):
                            pl.semaphore_wait(ready_sem.at[known - 1], row)
                            send_parts(known)
                            if (zz, known) == (mid, mid + 1):
                                send_part(zz, 1 - col)
                    issue(zz, item)

    def pack_rest():
        for turn in range(2, n):
            fill(turn)

        @pl.when(jnp.logical_not(central))
        def _():
            far = spill_starts(far_first)
            for o in range(spilled):
                at = DIRECT + o
                for j in range(1, half):
                    at = jnp.where(o >= far[j][0], j * MAXP + DIRECT + o - far[j][0], at)
                spill[o] = send[far_first * MAXP + jnp.minimum(at, half * MAXP - 1)]

    for turn in range(2):
        fill(turn)

    @pl.when(jnp.logical_not(central))
    def _():
        pack_rest()

    greeted = z * row + row - 1 + jnp.where(z == mid - 1, subs, 0)
    pl.semaphore_wait(barrier, jnp.where(z == mid, z * subs + subs - 1, greeted))

    for level in (mid - 1, mid):
        issue_early(level)

    @pl.when(z == mid - 1)
    def _():
        for spot in range(subs):
            for level, place in ((mid, col), (mid - 1, 1 - col)):
                pl.semaphore_signal(
                    mate_sem, inc=1, device_id=device(level, place * subs + spot),
                    device_id_type=MESH)

    @pl.when(z != mid)
    def _():
        tell_lower()

    @pl.when(central)
    def _():
        pack_rest()
    for level in range(line):
        if level not in (mid - 1, mid):
            issue_early(level)

    lane = lax.broadcasted_iota(jnp.int32, (layers, LANES), 1)
    for dest in range(n):
        total = jnp.zeros((layers, LANES), jnp.float32)
        for k in range(MAXP):
            v = send[dest * MAXP + k].astype(jnp.float32)
            s = jnp.sum(v * v, axis=1, keepdims=True)
            total = jnp.where(lane == k, s, total)
        part[dest] = total
    mine = pl.ds(pl.multiple_of(me * piece, LANES), piece)
    for k in range(MAXP):
        out[k, :, mine] = send[me * MAXP + k]
    parts_in[me] = part[me]

    @pl.when(central)
    def _():
        pl.semaphore_wait(mate_sem, subs)

    @pl.when(z == mid)
    def _():
        tell_lower()

    for level in range(line):
        @pl.when(z == level)
        def _():
            sends_later(level)

    whole(parts_in.at[pl.ds(0, n - 1)], precv_sem).wait()
    sums[0] = jnp.sum(parts_in[...], axis=0)
    pair = pltpu.make_async_remote_copy(
        src_ref=sums.at[0],
        dst_ref=sums.at[1],
        send_sem=send_sem,
        recv_sem=pair_sem,
        device_id={"sub": 1 - sub},
        device_id_type=MESH)
    pair.start()
    pair.wait_recv()
    total = sums[0] + sums[1]
    chk[...] = jnp.sqrt(1.0 + total / (PAGE * LATENT))[:, :MAXP]
    whole(parts_in, send_sem).wait()
    for level in range(line):
        away = away_of(level)
        forwards = 0 if away else mid - 1
        sent = (half - 1) * MAXP + half * kept_direct(away)
        got = (n - 1) * MAXP - forwards * rest

        @pl.when(z == level)
        def _():
            whole(send.at[pl.ds(0, sent)], send_sem).wait()
            if away:
                whole(spill, send_sem).wait()
            else:
                whole(send.at[pl.ds(0, forwards * (half - 1) * rest)], send_sem).wait()
            whole(send.at[pl.ds(0, got)], recv_sem).wait()


def place(pages_in, sums_in, pages, sums, sem):
    copies = [pltpu.make_async_copy(a, b, sem) for a, b in (
        (pages_in, pages), (sums_in, sums))]
    for copy in copies:
        copy.start()
    for copy in copies:
        copy.wait()


def direct(cache_in, page_counts, tail_tokens, assignment):
    n, subs = lax.axis_size("seq"), lax.axis_size("sub")
    pages, layers, piece = cache_in.shape
    mid = n // ROW_CHIPS // 2
    spilled = most_spilled(pages, n)
    vmem = pl.BlockSpec(memory_space=pltpu.VMEM)
    landed = pl.pallas_call(
        functools.partial(exchange, n, subs),
        out_shape=(pltpu.VMEM((MAXP, layers, piece * n), cache_in.dtype),
                   pltpu.VMEM((layers, MAXP), jnp.float32)),
        in_specs=[pl.BlockSpec(memory_space=pl.ANY)] * 4,
        out_specs=(vmem, vmem),
        scratch_shapes=[
            pltpu.VMEM((n * MAXP, layers, piece), cache_in.dtype),
            pltpu.VMEM((piece // LATENT + 1, layers, piece), cache_in.dtype),
            pltpu.VMEM((n, layers, LANES), jnp.float32),
            pltpu.VMEM((n, layers, LANES), jnp.float32),
            pltpu.SemaphoreType.DMA,
            pltpu.SemaphoreType.DMA,
            pltpu.SemaphoreType.DMA,
            pltpu.SemaphoreType.REGULAR((n // ROW_CHIPS - 1,)),
            pltpu.SemaphoreType.REGULAR,
            pltpu.SemaphoreType.DMA,
            pltpu.VMEM((2, layers, LANES), jnp.float32),
            pltpu.VMEM(cache_in.shape, cache_in.dtype),
            pltpu.SMEM(page_counts.shape, jnp.int32),
            pltpu.SMEM(page_counts.shape, jnp.int32),
            pltpu.SMEM(page_counts.shape, jnp.int32),
            pltpu.SemaphoreType.DMA((mid - 1,)),
            pltpu.VMEM((mid - 1, n // 2 * (MAXP - DIRECT), layers, piece), cache_in.dtype),
            pltpu.VMEM((spilled, layers, piece), cache_in.dtype),
        ] + [pltpu.VMEM((spilled + 1, layers, piece), cache_in.dtype)] * (mid - 1),
        compiler_params=pltpu.CompilerParams(collective_id=0, has_side_effects=True),
    )(page_counts, tail_tokens, assignment, cache_in)
    return pl.pallas_call(
        place,
        out_shape=tuple(jax.ShapeDtypeStruct(a.shape, a.dtype) for a in landed),
        in_specs=[vmem] * 2,
        out_specs=(pl.BlockSpec(memory_space=pltpu.HBM),) * 2,
        scratch_shapes=[pltpu.SemaphoreType.DMA],
    )(*(pltpu.with_memory_space_constraint(a, pltpu.VMEM) for a in landed))


def shards(cache_in, page_counts, tail_tokens, assignment):
    pages, _, piece = cache_in.shape
    n, subs = lax.axis_size("seq"), lax.axis_size("sub")
    whole_tiles = piece % LANES == 0 and piece % LATENT == 0
    in_order = n == len(ORDER) * ROW_CHIPS and subs == 2 and subs * ROW_CHIPS == len(ORDER[0])
    fits = in_order and page_counts.shape[0] == n
    return (direct if whole_tiles and fits else general)(cache_in, page_counts, tail_tokens, assignment)


def solution(mesh):
    placed = (P("groups", None, ("sub", "seq")), P("groups"), P("groups"), P("groups"))
    return jax.shard_map(
        shards,
        mesh=mesh,
        in_specs=placed,
        out_specs=(P(("groups", "seq"), None, "sub"), P(None, ("groups", "seq"))),
        check_vma=False,
    )
```
